256 devices in a mesh: fsdp: 16 (over x_hi, y, core), cp: 16 (over x_lo, z).
Axes of the slice: x: 4 (x_hi: 2, x_lo: 2; x = x_hi * 2 + x_lo), y: 4, z: 8, core: 2. Of those that a mesh axis runs over, the one named last changes fastest.
Arguments:
- features: bfloat16 [16, 2048, 2560], P('fsdp', 'cp'), may hold values from -6 to 6
- query_rows: bfloat16 [16, 2048, 1280], P('fsdp', 'cp'), may hold values from -40 to 40, as said below
- key_rows: bfloat16 [16, 2048, 1280], P('fsdp', 'cp'), may hold values from -4 to 4
- value_rows: bfloat16 [16, 2048, 1280], P('fsdp', 'cp'), may hold values from -6 to 6
- attn_output: bfloat16 [16, 2048, 1280], P('fsdp', 'cp'), may hold values from -6 to 6
- grad_output: bfloat16 [16, 2048, 1280], P('fsdp', 'cp'), may hold values from -6 to 6
- log_sums: float32 [16, 2048, 10], P('fsdp', 'cp'), as said below
Outputs:
- d_query: bfloat16 [16, 2048, 1280], P('fsdp', 'cp')
- d_key: bfloat16 [16, 2048, 1280], P('fsdp', 'cp')
- d_value: bfloat16 [16, 2048, 1280], P('fsdp', 'cp')
- d_value_weight: float32 [2560, 1280], P('fsdp', 'cp')
The draws below stay inside these ranges and needn't reach their ends.
Inputs may be any that keep to these rules, and one draw needn't show every extreme that they name: `query_rows`: queries of a clip, with key_rows and log_sums drawn together with them. log_sums[c, t, h] is the logarithm of the sum over all 2048 keys u of clip c of exp(128**-0.5 * q[t] . k[u]) for head h, computed from the bfloat16 queries and keys in float32.
All inputs are finite; a program needn't handle non-finite values.
Results may differ from the reference program's by a relative error of at most 0.02.
Values may be sent and summed in bfloat16 or wider, within the bound.
A program may use at most 128 MiB of HBM per device.

```python
import jax
import jax.numpy as jnp
from jax import lax

D = 2560
HEADS = 10
HEAD = 128
TOK_DEV = 128
CLIPS = 16
SEQ = 2048
QKV_WIDTH = 1280
N_CP = 16


def pair_draw(key):
    query_key = jax.random.fold_in(key, 101)
    key_key = jax.random.fold_in(key, 202)
    full_shape = (CLIPS, SEQ, HEADS * HEAD)
    key_vals = jax.random.truncated_normal(key_key, -4.0, 4.0, full_shape, jnp.float32)
    query_vals = jax.random.truncated_normal(query_key, -4.0, 4.0, full_shape, jnp.float32)
    query_half = query_vals.astype(jnp.bfloat16)
    key_half = key_vals.astype(jnp.bfloat16)
    query_side = query_half.astype(jnp.float32)
    key_side = key_half.astype(jnp.float32)

    def clip_norms(operands):
        query_heads = operands[0].reshape(SEQ, HEADS, HEAD)
        key_heads = operands[1].reshape(SEQ, HEADS, HEAD)
        scores = jnp.einsum('qhd,khd->hqk', query_heads, key_heads, precision=lax.Precision.HIGHEST) * HEAD ** (-0.5)
        return jax.nn.logsumexp(scores, axis=2).T
    log_norms = lax.map(clip_norms, (query_side, key_side)).astype(jnp.float32)
    return (query_half, key_half, log_norms)


def draw_query_rows(key, part):
    return pair_draw(key)[0]


def draw_key_rows(key, part):
    return pair_draw(key)[1]


def draw_log_sums(key, part):
    return pair_draw(key)[2]


def strengthened(drawn, own_key, source, target, parts, factor):
    def block_of(position):
        return (jnp.arange(drawn.shape[position]) // (drawn.shape[position] // parts)).reshape((-1,) + (1,) * (drawn.ndim - 1 - position))

    first = jax.random.permutation(own_key, parts)[block_of(target)]
    other_side = (block_of(target) + parts // 2) % parts
    return jnp.where((block_of(source) == first) | (block_of(source) == other_side), factor * drawn, drawn)


def shard_levels(stream_key, dims, shards, smallest, top_value):
    def one(position, shards_of):
        heights = jax.random.uniform(jax.random.fold_in(jax.random.fold_in(stream_key, 6), position), (shards_of,), jnp.float32, smallest / len(shards), top_value / len(shards))
        return jnp.repeat(jnp.exp(heights), dims[position] // shards_of).reshape((-1,) + (1,) * (len(dims) - position - 1))

    loudness = one(*shards[0])
    for cut in shards[1:]:
        loudness = loudness * one(*cut)
    return loudness


def normal_values(key, shape, width, limit, pieces=(), dtype=jnp.bfloat16):
    values = width * jax.random.normal(key, shape, jnp.float32)
    if pieces:
        values = values * shard_levels(key, shape, pieces, -0.22, 0.18)
    return jnp.clip(values, -limit, limit).astype(dtype)


def noise_with(rng, extent, deviation, most, pieces, heavy, dtype=jnp.bfloat16):
    values = deviation * jax.random.normal(rng, extent, jnp.float32)
    if pieces:
        values = values * shard_levels(rng, extent, pieces, -0.22, 0.18)
    return jnp.clip(strengthened(values, jax.random.fold_in(rng, 3), *heavy), -most, most).astype(dtype)


def setup_inputs(seed: int = 0) -> dict:
    seeds = jax.random.split(jax.random.key(seed), 8)
    features = noise_with(seeds[0], (CLIPS, SEQ, D), 1.0, 6.0, ((0, 16), (1, 16)), (0, 2, 16, 2.0))
    query_rows = draw_query_rows(jax.random.fold_in(seeds[7], 71), 0)
    key_rows = draw_key_rows(jax.random.fold_in(seeds[7], 71), 0)
    value_rows = normal_values(seeds[3], (CLIPS, SEQ, QKV_WIDTH), 1.0, 6.0, ((0, 16), (1, 16)))
    attn_output = normal_values(seeds[4], (CLIPS, SEQ, QKV_WIDTH), 1.0, 6.0, ((0, 16), (1, 16)))
    grad_output = normal_values(seeds[5], (CLIPS, SEQ, QKV_WIDTH), 1.0, 6.0, ((0, 16), (1, 16)))
    log_sums = draw_log_sums(jax.random.fold_in(seeds[7], 71), 0)
    return {"features": features, "query_rows": query_rows, "key_rows": key_rows, "value_rows": value_rows, "attn_output": attn_output, "grad_output": grad_output, "log_sums": log_sums}


def split_heads(matrix):
    return matrix.reshape(matrix.shape[0], HEADS, HEAD).astype(jnp.float32)


def clip_backward(operands):
    queries, key_side, value_side, attn_out, grad_out, log_norm, inputs = operands
    softmax_scale = HEAD ** -0.5
    query_heads = split_heads(queries)
    key_heads = split_heads(key_side)
    value_heads = split_heads(value_side)
    grad_heads = split_heads(grad_out)
    row_delta = jnp.sum(grad_heads * split_heads(attn_out), axis=2)
    scores = jnp.einsum("qhd,khd->hqk", query_heads, key_heads) * softmax_scale
    attn_prob = jnp.exp(scores - log_norm.T[:, :, None])
    grad_prob = jnp.einsum("qhd,khd->hqk", grad_heads, value_heads)
    grad_score = (attn_prob * (grad_prob - row_delta.T[:, :, None])).astype(jnp.bfloat16)
    grad_score = lax.optimization_barrier(grad_score).astype(jnp.float32)
    grad_query = softmax_scale * jnp.einsum("hqk,khd->qhd", grad_score, key_heads)
    grad_key = softmax_scale * jnp.einsum("hqk,qhd->khd", grad_score, query_heads)
    prob_rounded = lax.optimization_barrier(attn_prob.astype(jnp.bfloat16)).astype(jnp.float32)
    grad_value = jnp.einsum("hqk,qhd->khd", prob_rounded, grad_heads)
    grad_query = grad_query.reshape(SEQ, QKV_WIDTH).astype(jnp.bfloat16)
    grad_key = grad_key.reshape(SEQ, QKV_WIDTH).astype(jnp.bfloat16)
    grad_value = grad_value.reshape(SEQ, QKV_WIDTH).astype(jnp.bfloat16)
    feature_blocks = inputs.reshape(N_CP, TOK_DEV, D)
    value_blocks = grad_value.reshape(N_CP, TOK_DEV, QKV_WIDTH)

    def add_block(running, blocks):
        block_term = jnp.dot(blocks[0].T, blocks[1], preferred_element_type=jnp.float32)
        rounded = lax.optimization_barrier(block_term.astype(jnp.bfloat16)).astype(jnp.float32)
        return running + rounded, None

    weight_sum, _ = lax.scan(add_block, jnp.zeros((D, QKV_WIDTH), jnp.float32), (feature_blocks, value_blocks))
    return grad_query, grad_key, grad_value, weight_sum


def reference(features, query_rows, key_rows, value_rows, attn_output, grad_output, log_sums):
    results = lax.map(clip_backward, (query_rows, key_rows, value_rows, attn_output, grad_output, log_sums, features))
    return results[0], results[1], results[2], jnp.sum(results[3], axis=0)
```

```python
import functools

import jax
import jax.numpy as jnp
from jax import lax
from jax.experimental import pallas as pl
from jax.experimental.pallas import tpu as pltpu
from jax.sharding import Mesh
from jax.sharding import PartitionSpec as P

AXES = ("x_hi", "y", "core", "x_lo", "z")
FSDP = ("x_hi", "y", "core")
CP = ("x_lo", "z")
LOG2E = 1.4426950408889634
HEADS = 10
N_CP = 16
N_Z = 8
MESH = pl.DeviceIdType.MESH


def owner_of(head, parity):
    spare = head >= N_Z
    z = jnp.where(spare, 2 * parity + 4 * (head - N_Z), head)
    x = jnp.where(spare, 1 - parity, lax.rem(head + parity, 2))
    return x, z


def head_of(x, z, parity):
    first = x == lax.rem(z + parity, 2)
    spare = jnp.where(z == 2 * parity, N_Z, jnp.where(z == 2 * parity + 4, N_Z + 1, HEADS))
    return jnp.where(first, z, spare)


def attend_kernel(
    q_in, k_in, v_in, g_in, s_in, dq_out, dk_out, dv_out,
    q_buf, k_buf, v_buf, g_buf, s_buf, dq_acc, dk_acc, dv_acc, done, back,
    send_sem, recv_sem, ret_send, ret_recv, out_sem, *, scale, rows
):
    x, z, parity = lax.axis_index("x_lo"), lax.axis_index("z"), lax.axis_index("core")
    me = x * N_Z + z
    mine = head_of(x, z, parity)
    active = mine < HEADS
    span = 128

    barrier = pltpu.get_barrier_semaphore()

    def greet(j, _):
        peer = lax.rem(me + j, N_CP)
        pl.semaphore_signal(
            barrier, inc=1,
            device_id={"x_lo": peer // N_Z, "z": lax.rem(peer, N_Z)}, device_id_type=MESH)
        return 0

    lax.fori_loop(1, N_CP, greet, 0)
    pl.semaphore_wait(barrier, N_CP - 1)

    ins = (k_in, q_in, v_in, g_in)
    bufs = (k_buf, q_buf, v_buf, g_buf)

    def sources(head):
        cols = pl.ds(pl.multiple_of(head * span, span), span)
        return [a.at[0, :, cols] for a in ins] + [s_in.at[head]]

    def targets(block):
        return [b.at[block] for b in bufs] + [s_buf.at[block]]

    def head_at(i):
        off = jnp.where(lax.rem(i, 2) == 0, i // 2 + 1, jnp.where(i == 7, 0, N_Z - (i + 1) // 2))
        return jnp.where(i < N_Z, lax.rem(z + off, N_Z), i)

    def send(i, _):
        head = head_at(i)
        ox, oz = owner_of(head, parity)
        away = head != mine

        @pl.when(away)
        def _():
            for t, (src, dst) in enumerate(zip(sources(head), targets(me))):
                pltpu.make_async_remote_copy(
                    src_ref=src, dst_ref=dst, send_sem=send_sem.at[t, head],
                    recv_sem=recv_sem.at[t, me], device_id={"x_lo": ox, "z": oz},
                    device_id_type=MESH).start()

        @pl.when(jnp.logical_not(away))
        def _():
            for t, (src, dst) in enumerate(zip(sources(head), targets(me))):
                pltpu.make_async_copy(src, dst, recv_sem.at[t, me]).start()

        return 0

    lax.fori_loop(0, HEADS, send, 0)

    @pl.when(active)
    def _():
        def arrive(r, _):
            for t, (src, dst) in enumerate(zip(sources(0), targets(r))):
                pltpu.make_async_copy(src, dst, recv_sem.at[t, r]).wait()
            return 0

        lax.fori_loop(0, N_CP, arrive, 0)
        dk_acc[...] = jnp.zeros_like(dk_acc)
        dv_acc[...] = jnp.zeros_like(dv_acc)
        TB, UB = 4, 4

        def query_step(tb, _):
            qs = pl.ds(tb * TB, TB)
            q = q_buf[qs].reshape(TB * rows, span)
            g = g_buf[qs].reshape(TB * rows, span)
            lse = jnp.concatenate([s_buf[tb * TB + i, 0:1, :] for i in range(TB)], axis=1)
            delta = jnp.concatenate([s_buf[tb * TB + i, 1:2, :] for i in range(TB)], axis=1)

            def key_step(ub, dq):
                us = pl.ds(ub * UB, UB)
                k = k_buf[us].reshape(UB * rows, span)
                v = v_buf[us].reshape(UB * rows, span)
                nt = (((1,), (1,)), ((), ()))
                st = lax.dot_general(k, q, nt, preferred_element_type=jnp.float32)
                prob = jnp.exp2(st * (scale * LOG2E) - lse)
                dp = lax.dot_general(v, g, nt, preferred_element_type=jnp.float32)
                ds = (prob * (dp - delta)).astype(jnp.bfloat16)
                p16 = prob.astype(jnp.bfloat16)
                dv = jnp.dot(p16, g, preferred_element_type=jnp.float32)
                dk = jnp.dot(ds, q, preferred_element_type=jnp.float32)
                rs = pl.ds(pl.multiple_of(ub * UB * rows, UB * rows), UB * rows)
                dv_acc[rs, :] += dv
                dk_acc[rs, :] += dk
                return dq + lax.dot_general(
                    ds, k, (((0,), (0,)), ((), ())), preferred_element_type=jnp.float32)

            dq = lax.fori_loop(0, N_CP // UB, key_step, jnp.zeros((TB * rows, span), jnp.float32))
            dq_acc[pl.ds(pl.multiple_of(tb * TB * rows, TB * rows), TB * rows), :] = dq
            return 0

        lax.fori_loop(0, N_CP // TB, query_step, 0)
        done[0] = dv_acc[...].astype(jnp.bfloat16).reshape(N_CP, rows, span)
        done[1] = (dk_acc[...] * scale).astype(jnp.bfloat16).reshape(N_CP, rows, span)
        done[2] = (dq_acc[...] * scale).astype(jnp.bfloat16).reshape(N_CP, rows, span)

        cols = pl.ds(pl.multiple_of(mine * span, span), span)
        for t in range(3):
            def give(j, _):
                peer = lax.rem(me + j, N_CP)
                pltpu.make_async_remote_copy(
                    src_ref=done.at[t, peer], dst_ref=back.at[t, :, cols],
                    send_sem=ret_send.at[t, peer], recv_sem=ret_recv.at[t, mine],
                    device_id={"x_lo": peer // N_Z, "z": lax.rem(peer, N_Z)},
                    device_id_type=MESH).start()
                return 0

            lax.fori_loop(1, N_CP, give, 0)
            back[t, :, cols] = done[t, me]

    outs = (dv_out, dk_out, dq_out)
    for t in range(3):
        def collect(h, _):
            @pl.when(h != mine)
            def _():
                cols = pl.ds(pl.multiple_of(h * span, span), span)
                pltpu.make_async_copy(done.at[t, 0], back.at[t, :, cols], ret_recv.at[t, h]).wait()
            return 0

        lax.fori_loop(0, HEADS, collect, 0)
        pltpu.make_async_copy(back.at[t], outs[t].at[0], out_sem.at[t]).start()

    def sent(head, _):
        @pl.when(head != mine)
        def _():
            for t, (src, dst) in enumerate(zip(sources(head), targets(me))):
                pltpu.make_async_copy(src, dst, send_sem.at[t, head]).wait()
        return 0

    lax.fori_loop(0, HEADS, sent, 0)

    @pl.when(active)
    def _():
        def gave(j, _):
            peer = lax.rem(me + j, N_CP)
            for t in range(3):
                pltpu.make_async_copy(
                    done.at[t, peer], done.at[t, peer], ret_send.at[t, peer]).wait()
            return 0

        lax.fori_loop(1, N_CP, gave, 0)

    for t in range(3):
        pltpu.make_async_copy(back.at[t], outs[t].at[0], out_sem.at[t]).wait()


def attend(q, k, v, g, stats):
    _, rows, width = q.shape
    any_spec = pl.BlockSpec(memory_space=pl.ANY)
    block = pltpu.VMEM((N_CP, rows, 128), jnp.bfloat16)
    acc = pltpu.VMEM((N_CP * rows, 128), jnp.float32)
    out = jax.ShapeDtypeStruct(q.shape, jnp.bfloat16)
    return pl.pallas_call(
        functools.partial(attend_kernel, scale=128**-0.5, rows=rows),
        out_shape=(out, out, out),
        in_specs=[any_spec] * 5,
        out_specs=(any_spec,) * 3,
        scratch_shapes=[
            block, block, block, block,
            pltpu.VMEM((N_CP, 8, rows), jnp.float32),
            acc, acc, acc,
            pltpu.VMEM((3, N_CP, rows, 128), jnp.bfloat16),
            pltpu.VMEM((3, rows, width), jnp.bfloat16),
            pltpu.SemaphoreType.DMA((5, HEADS)),
            pltpu.SemaphoreType.DMA((5, N_CP)),
            pltpu.SemaphoreType.DMA((3, N_CP)),
            pltpu.SemaphoreType.DMA((3, HEADS)),
            pltpu.SemaphoreType.DMA((3,)),
        ],
        compiler_params=pltpu.CompilerParams(collective_id=0, has_side_effects=True),
        name="attend",
    )(q, k, v, g, stats)


def reduced_to_own(pieces, axes, sequence):
    inside = pieces.shape[1:]
    pieces = pieces.reshape(*(lax.axis_size(a) for a in axes), *inside)
    pieces = jnp.moveaxis(pieces, sequence, range(len(axes))).reshape(-1, *inside)
    for k in sequence:
        pieces = lax.psum_scatter(pieces, axes[k], scatter_dimension=0, tiled=True)
    return pieces[0]


def cut_along(array, dim, size):
    before, after = (array.shape[:dim], array.shape[dim + 1 :])
    return jnp.moveaxis(array.reshape(*before, size, -1, *after), dim, 0)


def on_device(features, query_rows, key_rows, value_rows, attn_output, grad_output, log_sums):
    rows = query_rows.shape[1]
    product = grad_output.astype(jnp.float32) * attn_output.astype(jnp.float32)
    delta = jnp.sum(product.reshape(rows, HEADS, 128), axis=2).T
    lse = log_sums[0].T * LOG2E
    stats = jnp.stack([lse, delta] + [jnp.zeros_like(lse)] * 6, axis=1)
    d_query, d_key, d_value = attend(query_rows, key_rows, value_rows, grad_output, stats)
    weight_term = jnp.einsum(
        "tf,tw->fw", features[0], d_value[0], preferred_element_type=jnp.float32
    )
    pieces = cut_along(weight_term.astype(jnp.bfloat16), 1, N_CP)
    column_part = reduced_to_own(pieces, CP, (1, 0))
    pieces = cut_along(column_part, 0, 16)
    arrived = lax.all_to_all(pieces, FSDP, split_axis=0, concat_axis=0, tiled=True)
    return d_query, d_key, d_value, arrived.astype(jnp.float32).sum(axis=0)


def solution(mesh):
    finer = Mesh(mesh.devices.reshape(2, 4, 2, 2, 8), AXES)
    rows = P(FSDP, CP, None)
    return jax.shard_map(
        on_device, mesh=finer, in_specs=(rows,) * 7,
        out_specs=(rows, rows, rows, P(FSDP, CP)), check_vma=False,
    )
```

```python
import functools

import jax
import jax.numpy as jnp
from jax import lax
from jax.experimental import pallas as pl
from jax.experimental.pallas import tpu as pltpu
from jax.sharding import Mesh
from jax.sharding import PartitionSpec as P

AXES = ("x_hi", "y", "core", "x_lo", "z")
FSDP = ("x_hi", "y", "core")
CP = ("x_lo", "z")
LOG2E = 1.4426950408889634
HEADS = 10
SPAN = 128
N_CP = 16
N_Z = 8
MESH = pl.DeviceIdType.MESH
F32 = jnp.float32
BF16 = jnp.bfloat16
NT = (((1,), (1,)), ((), ()))
TN = (((0,), (0,)), ((), ()))


def owner_of(head, parity):
    spare = head >= N_Z
    z = jnp.where(spare, 2 * parity + 4 * (head - N_Z), head)
    x = jnp.where(spare, 1 - parity, lax.rem(head + parity, 2))
    return x, z


def head_of(x, z, parity):
    first = x == lax.rem(z + parity, 2)
    spare = jnp.where(z == 2 * parity, N_Z, jnp.where(z == 2 * parity + 4, N_Z + 1, HEADS))
    return jnp.where(first, z, spare)


def step_kernel(
    f_in, q_in, k_in, v_in, o_in, g_in, l_in, dq_out, dk_out, dv_out, dw_out,
    q_buf, k_buf, v_buf, g_buf, s_buf, prob, dq_acc, done, back,
    g_own, o_own, l_own, s_own, f_own, ft_own, ft_buf, dv_buf,
    half_send, half_recv, part, x_send, x_recv, z_send, z_recv, total,
    in_sem, send_sem, recv_sem, ret_send, ret_recv, out_sem,
    f_ssem, f_rsem, y_ssem, y_rsem, d_ssem, d_rsem, x_ssem, x_rsem, z_ssem, z_rsem,
    *, scale, rows
):
    xh, y, core = lax.axis_index("x_hi"), lax.axis_index("y"), lax.axis_index("core")
    xl, z = lax.axis_index("x_lo"), lax.axis_index("z")
    x = 2 * xh + xl
    me = xl * N_Z + z
    mine = head_of(xl, z, core)
    active = mine < HEADS
    feat = f_in.shape[2]
    half_f, quarter_f = feat // 2, feat // 4
    half_w = q_in.shape[2] // 2
    blk = quarter_f // 4
    col = half_w // N_Z

    def cp_id(peer):
        return {"x_lo": peer // N_Z, "z": lax.rem(peer, N_Z)}

    def x_id(p):
        return {"x_hi": p // 2, "x_lo": lax.rem(p, 2)}

    to_xh, to_xl, to_y, to_core = y // 2, lax.rem(y, 2), 2 * core + xh, xl
    from_y, from_core, from_xh, from_xl = 2 * xh + xl, y // 2, lax.rem(y, 2), core
    loop = jnp.logical_and(
        jnp.logical_and(to_xh == xh, to_xl == xl), jnp.logical_and(to_y == y, to_core == core))

    def to_id(zz):
        return {"x_hi": to_xh, "y": to_y, "core": to_core, "x_lo": to_xl, "z": zz}

    loads = [
        pltpu.make_async_copy(g_in.at[0], g_own, in_sem.at[0]),
        pltpu.make_async_copy(o_in.at[0], o_own, in_sem.at[1]),
        pltpu.make_async_copy(l_in.at[0], l_own, in_sem.at[2]),
        pltpu.make_async_copy(f_in.at[0], f_own, in_sem.at[3]),
    ]
    for c in loads:
        c.start()

    barrier = pltpu.get_barrier_semaphore()

    def signal(where):
        pl.semaphore_signal(barrier, inc=1, device_id=where, device_id_type=MESH)

    def greet_cp(j, _):
        signal(cp_id(lax.rem(me + j, N_CP)))
        return 0

    def greet_quad(j, _):
        signal({"y": lax.rem(y + j, 4)})
        signal(x_id(lax.rem(x + j, 4)))
        return 0

    def greet_from(zz, _):
        @pl.when(jnp.logical_not(jnp.logical_and(loop, zz == z)))
        def _():
            signal({"x_hi": from_xh, "y": from_y, "core": from_core, "x_lo": from_xl, "z": zz})
        return 0

    lax.fori_loop(0, N_Z, greet_from, 0)
    lax.fori_loop(1, N_CP, greet_cp, 0)
    lax.fori_loop(1, 4, greet_quad, 0)
    signal({"core": 1 - core})
    pl.semaphore_wait(barrier, jnp.where(loop, 29, 30))

    def head_at(i):
        off = jnp.where(lax.rem(i, 2) == 0, i // 2 + 1, jnp.where(i == 7, 0, N_Z - (i + 1) // 2))
        return jnp.where(i < N_Z, lax.rem(z + off, N_Z), i)

    def cols_of(head):
        return pl.ds(pl.multiple_of(head * SPAN, SPAN), SPAN)

    ins = (k_in, q_in, g_in, v_in)
    bufs = (k_buf, q_buf, g_buf, v_buf)

    def source(t, head):
        return ins[t].at[0, :, cols_of(head)] if t < 4 else s_own.at[head]

    def target(t, block):
        return bufs[t].at[block] if t < 4 else s_buf.at[block]

    def send_all(kinds):
        def send(i, _):
            head = head_at(i)
            ox, oz = owner_of(head, core)

            @pl.when(head != mine)
            def _():
                for t in kinds:
                    pltpu.make_async_remote_copy(
                        src_ref=source(t, head), dst_ref=target(t, me),
                        send_sem=send_sem.at[t, head], recv_sem=recv_sem.at[t, me],
                        device_id={"x_lo": ox, "z": oz}, device_id_type=MESH).start()

            @pl.when(head == mine)
            def _():
                for t in kinds:
                    if t < 4:
                        pltpu.make_async_copy(source(t, head), target(t, me), recv_sem.at[t, me]).start()
                    else:
                        s_buf[me] = s_own[head]

            return 0

        lax.fori_loop(0, HEADS, send, 0)

    send_all((0, 1, 2))

    for c in loads[:3]:
        c.wait()
    lse = jnp.concatenate([l_own[...] * LOG2E, jnp.zeros((rows, SPAN - HEADS), F32)], axis=1).T
    s_own[...] = jnp.zeros_like(s_own)
    for h in range(HEADS):
        hs = slice(h * SPAN, (h + 1) * SPAN)
        product = g_own[:, hs].astype(F32) * o_own[:, hs].astype(F32)
        s_own[h, 0:1, :] = lse[h : h + 1]
        s_own[h, 1:2, :] = jnp.sum(product.T, axis=0, keepdims=True)
    send_all((4, 3))

    loads[3].wait()

    def turn(i, _):
        at = pl.multiple_of(i * SPAN, SPAN)
        ft_own[pl.ds(at, SPAN), :] = f_own[:, pl.ds(at, SPAN)].T
        return 0

    lax.fori_loop(0, feat // SPAN, turn, 0)
    my_rows = pl.ds(pl.multiple_of(y * SPAN, SPAN), SPAN)

    def feature_copy(j):
        to = lax.rem(y + j, 4)
        start = pl.multiple_of((to // 2) * half_f, half_f)
        return pltpu.make_async_remote_copy(
            src_ref=ft_own.at[pl.ds(start, half_f), :], dst_ref=ft_buf.at[:, my_rows],
            send_sem=f_ssem.at[j], recv_sem=f_rsem.at[j], device_id={"y": to},
            device_id_type=MESH)

    for j in range(1, 4):
        feature_copy(j).start()
    ft_buf[:, my_rows] = ft_own[pl.ds(pl.multiple_of((y // 2) * half_f, half_f), half_f), :]

    @pl.when(active)
    def _():
        def arrive(kinds):
            def one(r, _):
                for t in kinds:
                    if t < 4:
                        pltpu.make_async_copy(source(t, 0), target(t, r), recv_sem.at[t, r]).wait()
                    else:
                        @pl.when(r != me)
                        def _():
                            pltpu.make_async_copy(source(t, 0), target(t, r), recv_sem.at[t, r]).wait()
                return 0
            lax.fori_loop(0, N_CP, one, 0)

        arrive((0, 1, 2, 4))
        UB = 2
        seq = N_CP * rows
        q = q_buf[...].reshape(seq, SPAN)
        g = g_buf[...].reshape(seq, SPAN)
        lse = jnp.concatenate([s_buf[i, 0:1, :] for i in range(N_CP)], axis=1)
        delta = jnp.concatenate([s_buf[i, 1:2, :] for i in range(N_CP)], axis=1)

        def value_step(ub, _):
            us = pl.ds(ub * UB, UB)
            k = k_buf[us].reshape(UB * rows, SPAN)
            st = lax.dot_general(k, q_buf[...].reshape(seq, SPAN), NT, preferred_element_type=F32)
            p = jnp.exp2(st * (scale * LOG2E) - lse)
            prob[pl.ds(pl.multiple_of(ub * UB * rows, UB * rows), UB * rows), :] = p
            dv = jnp.dot(p.astype(BF16), g_buf[...].reshape(seq, SPAN), preferred_element_type=F32)
            done[0, us] = dv.astype(BF16).reshape(UB, rows, SPAN)
            return 0

        lax.fori_loop(0, N_CP // UB, value_step, 0)

        def give_all(t):
            def give(j, _):
                peer = lax.rem(me + j, N_CP)
                pltpu.make_async_remote_copy(
                    src_ref=done.at[t, peer], dst_ref=back.at[t, :, cols_of(mine)],
                    send_sem=ret_send.at[t, peer], recv_sem=ret_recv.at[t, mine],
                    device_id=cp_id(peer), device_id_type=MESH).start()
                return 0

            lax.fori_loop(1, N_CP, give, 0)
            back[t, :, cols_of(mine)] = done[t, me]

        give_all(0)
        arrive((3,))
        dq_acc[...] = jnp.zeros_like(dq_acc)

        def key_step(ub, _):
            us = pl.ds(ub * UB, UB)
            k = k_buf[us].reshape(UB * rows, SPAN)
            v = v_buf[us].reshape(UB * rows, SPAN)
            p = prob[pl.ds(pl.multiple_of(ub * UB * rows, UB * rows), UB * rows), :]
            dp = lax.dot_general(v, g_buf[...].reshape(seq, SPAN), NT, preferred_element_type=F32)
            ds = (p * (dp - delta)).astype(BF16)
            dk = jnp.dot(ds, q_buf[...].reshape(seq, SPAN), preferred_element_type=F32)
            done[1, us] = (dk * scale).astype(BF16).reshape(UB, rows, SPAN)
            dq_acc[...] += lax.dot_general(ds, k, TN, preferred_element_type=F32)
            return 0

        lax.fori_loop(0, N_CP // UB, key_step, 0)
        give_all(1)
        done[2] = (dq_acc[...] * scale).astype(BF16).reshape(N_CP, rows, SPAN)
        give_all(2)

    outs = (dv_out, dk_out, dq_out)

    def collect_all(t):
        def collect(h, _):
            @pl.when(h != mine)
            def _():
                pltpu.make_async_copy(done.at[t, 0], back.at[t, :, cols_of(h)], ret_recv.at[t, h]).wait()
            return 0

        lax.fori_loop(0, HEADS, collect, 0)
        pltpu.make_async_copy(back.at[t], outs[t].at[0], out_sem.at[t]).start()

    collect_all(0)

    def value_copy(j):
        to = lax.rem(y + j, 4)
        cols = pl.ds(pl.multiple_of(lax.rem(to, 2) * half_w, half_w), half_w)
        return pltpu.make_async_remote_copy(
            src_ref=back.at[0, :, cols], dst_ref=dv_buf.at[my_rows, :],
            send_sem=y_ssem.at[j], recv_sem=y_rsem.at[j], device_id={"y": to},
            device_id_type=MESH)

    for j in range(1, 4):
        value_copy(j).start()
    dv_buf[my_rows, :] = back[0, :, pl.ds(pl.multiple_of(lax.rem(y, 2) * half_w, half_w), half_w)]
    for j in range(1, 4):
        feature_copy(j).wait()
    for j in range(1, 4):
        value_copy(j).wait()

    def part_of(which, p):
        at = pl.multiple_of(which * quarter_f + p * blk, blk)
        return jnp.dot(ft_buf[pl.ds(at, blk), :], dv_buf[...], preferred_element_type=F32)

    def half_copy(p):
        return pltpu.make_async_remote_copy(
            src_ref=half_send.at[p], dst_ref=half_recv.at[p], send_sem=d_ssem.at[p],
            recv_sem=d_rsem.at[p], device_id={"core": 1 - core}, device_id_type=MESH)

    def x_copy(j):
        to = lax.rem(x + j, 4)
        return pltpu.make_async_remote_copy(
            src_ref=x_send.at[j], dst_ref=x_recv.at[j], send_sem=x_ssem.at[j],
            recv_sem=x_rsem.at[j], device_id=x_id(to), device_id_type=MESH)

    order = (1, 2, 3, 0)
    for j in order:
        p = lax.rem(x + j, 4)
        half_send[p] = part_of(1 - core, p).astype(BF16)
        half_copy(p).start()
    for j in order:
        p = lax.rem(x + j, 4)
        part[...] = part_of(core, p)
        half_copy(p).wait_recv()
        both = part[...] + half_recv[p].astype(F32)
        if j:
            x_send[j] = both.astype(BF16)
            x_copy(j).start()
        else:
            part[...] = both
    both = part[...]
    for j in range(1, 4):
        x_copy(j).wait_recv()
        both += x_recv[j].astype(F32)

    gap = jnp.zeros((blk, SPAN - col), BF16)
    for zz in range(N_Z):
        piece = both[:, zz * col : (zz + 1) * col].astype(BF16)
        z_send[zz] = jnp.concatenate([piece, gap], axis=1)

    def z_copy(zz):
        return pltpu.make_async_remote_copy(
            src_ref=z_send.at[zz], dst_ref=z_recv.at[z], send_sem=z_ssem.at[zz],
            recv_sem=z_rsem.at[z], device_id=to_id(zz), device_id_type=MESH)

    def is_loop(zz):
        return jnp.logical_and(loop, zz == z)

    def z_start(i, _):
        zz = lax.rem(z + i, N_Z)

        @pl.when(jnp.logical_not(is_loop(zz)))
        def _():
            z_copy(zz).start()

        @pl.when(is_loop(zz))
        def _():
            z_recv[zz] = z_send[zz]

        return 0

    lax.fori_loop(0, N_Z, z_start, 0)
    collect_all(1)
    collect_all(2)
    total[...] = jnp.zeros_like(total)

    def z_take(zz, _):
        @pl.when(jnp.logical_not(is_loop(zz)))
        def _():
            pltpu.make_async_copy(z_send.at[zz], z_recv.at[zz], z_rsem.at[zz]).wait()

        total[...] += z_recv[zz][:, :col].astype(F32)
        return 0

    lax.fori_loop(0, N_Z, z_take, 0)
    last = pltpu.make_async_copy(total, dw_out, out_sem.at[3])
    last.start()

    def sent(head, _):
        @pl.when(head != mine)
        def _():
            for t in range(5):
                pltpu.make_async_copy(source(t, head), target(t, me), send_sem.at[t, head]).wait()
        return 0

    lax.fori_loop(0, HEADS, sent, 0)

    @pl.when(active)
    def _():
        def gave(j, _):
            peer = lax.rem(me + j, N_CP)
            for t in range(3):
                pltpu.make_async_copy(
                    done.at[t, peer], back.at[t, :, cols_of(mine)], ret_send.at[t, peer]).wait()
            return 0

        lax.fori_loop(1, N_CP, gave, 0)

    for p in range(4):
        half_copy(p).wait_send()
    for j in range(1, 4):
        x_copy(j).wait_send()

    def z_sent(zz, _):
        @pl.when(jnp.logical_not(is_loop(zz)))
        def _():
            z_copy(zz).wait_send()
        return 0

    lax.fori_loop(0, N_Z, z_sent, 0)
    for t in range(3):
        pltpu.make_async_copy(back.at[t], outs[t].at[0], out_sem.at[t]).wait()
    last.wait()


def on_device(features, query_rows, key_rows, value_rows, attn_output, grad_output, log_sums):
    _, rows, width = query_rows.shape
    feat = features.shape[2]
    seq = N_CP * rows
    blk, half_w = feat // 16, width // 2
    any_spec = pl.BlockSpec(memory_space=pl.ANY)
    block = pltpu.VMEM((N_CP, rows, SPAN), BF16)
    out = jax.ShapeDtypeStruct(query_rows.shape, BF16)
    dma = pltpu.SemaphoreType.DMA
    return pl.pallas_call(
        functools.partial(step_kernel, scale=SPAN**-0.5, rows=rows),
        out_shape=(out, out, out, jax.ShapeDtypeStruct((blk, half_w // N_Z), F32)),
        in_specs=[any_spec] * 7,
        out_specs=(any_spec,) * 4,
        scratch_shapes=[
            block, block, block, block,
            pltpu.VMEM((N_CP, 8, rows), F32),
            pltpu.VMEM((seq, seq), F32),
            pltpu.VMEM((seq, SPAN), F32),
            pltpu.VMEM((3, N_CP, rows, SPAN), BF16),
            pltpu.VMEM((3, rows, width), BF16),
            pltpu.VMEM((rows, width), BF16),
            pltpu.VMEM((rows, width), BF16),
            pltpu.VMEM((rows, HEADS), F32),
            pltpu.VMEM((HEADS, 8, rows), F32),
            pltpu.VMEM((rows, feat), BF16),
            pltpu.VMEM((feat, rows), BF16),
            pltpu.VMEM((feat // 2, 4 * rows), BF16),
            pltpu.VMEM((4 * rows, half_w), BF16),
            pltpu.VMEM((4, blk, half_w), BF16),
            pltpu.VMEM((4, blk, half_w), BF16),
            pltpu.VMEM((blk, half_w), F32),
            pltpu.VMEM((4, blk, half_w), BF16),
            pltpu.VMEM((4, blk, half_w), BF16),
            pltpu.VMEM((N_Z, blk, SPAN), BF16),
            pltpu.VMEM((N_Z, blk, SPAN), BF16),
            pltpu.VMEM((blk, half_w // N_Z), F32),
            dma((4,)),
            dma((5, HEADS)), dma((5, N_CP)), dma((3, N_CP)), dma((3, HEADS)), dma((4,)),
            dma((4,)), dma((4,)), dma((4,)), dma((4,)), dma((4,)), dma((4,)),
            dma((4,)), dma((4,)), dma((N_Z,)), dma((N_Z,)),
        ],
        compiler_params=pltpu.CompilerParams(
            collective_id=0, has_side_effects=True, vmem_limit_bytes=60 * 2**20),
        name="step",
    )(features, query_rows, key_rows, value_rows, attn_output, grad_output, log_sums)


def solution(mesh):
    finer = Mesh(mesh.devices.reshape(2, 4, 2, 2, 8), AXES)
    rows = P(FSDP, CP, None)
    return jax.shard_map(
        on_device, mesh=finer, in_specs=(rows,) * 7,
        out_specs=(rows, rows, rows, P(FSDP, CP)), check_vma=False,
    )
```

```python
import functools

import jax
import jax.numpy as jnp
from jax import lax
from jax.experimental import pallas as pl
from jax.experimental.pallas import tpu as pltpu
from jax.sharding import Mesh
from jax.sharding import PartitionSpec as P

AXES = ("x_hi", "y", "core", "x_lo", "z")
FSDP = ("x_hi", "y", "core")
CP = ("x_lo", "z")
LOG2E = 1.4426950408889634
HEADS = 10
SPAN = 128
N_CP = 16
N_Z = 8
MESH = pl.DeviceIdType.MESH
F32 = jnp.float32
BF16 = jnp.bfloat16
NT = (((1,), (1,)), ((), ()))
TN = (((0,), (0,)), ((), ()))


def owner_of(head, parity):
    spare = head >= N_Z
    z = jnp.where(spare, 2 * parity + 4 * (head - N_Z), head)
    x = jnp.where(spare, 1 - parity, lax.rem(head + parity, 2))
    return x, z


def head_of(x, z, parity):
    first = x == lax.rem(z + parity, 2)
    spare = jnp.where(z == 2 * parity, N_Z, jnp.where(z == 2 * parity + 4, N_Z + 1, HEADS))
    return jnp.where(first, z, spare)


def step_kernel(
    f_in, q_in, k_in, v_in, o_in, g_in, l_in, dq_out, dk_out, dv_out, dw_out,
    q_buf, k_buf, v_buf, g_buf, s_buf, prob, dq_acc, done, back,
    g_own, o_own, l_own, s_own, f_own, ft_own, ft_buf, dv_buf,
    half_send, half_recv, part, x_send, x_recv, z_send, z_recv, total,
    in_sem, send_sem, recv_sem, ret_send, ret_recv, out_sem,
    f_ssem, f_rsem, y_ssem, y_rsem, d_ssem, d_rsem, x_ssem, x_rsem, z_ssem, z_rsem,
    *, scale, rows
):
    xh, y, core = lax.axis_index("x_hi"), lax.axis_index("y"), lax.axis_index("core")
    xl, z = lax.axis_index("x_lo"), lax.axis_index("z")
    x = 2 * xh + xl
    me = 2 * z + xl
    mine = head_of(xl, z, core)
    active = mine < HEADS
    feat = f_in.shape[2]
    half_w = q_in.shape[2] // 2
    blk = feat // 16
    per = feat // 4 // SPAN
    col = half_w // N_Z

    def cp_id(peer):
        return {"x_lo": lax.rem(peer, 2), "z": peer // 2}

    y1, y0 = y // 2, lax.rem(y, 2)
    stays = y0 == xl

    def row_id(p):
        return {"x_hi": p // 2, "x_lo": lax.rem(p, 2)}

    def owner_id(zz):
        return {"x_lo": y0, "y": 2 * y1 + xl, "z": zz}

    loads = [
        pltpu.make_async_copy(g_in.at[0], g_own, in_sem.at[0]),
        pltpu.make_async_copy(o_in.at[0], o_own, in_sem.at[1]),
        pltpu.make_async_copy(l_in, l_own, in_sem.at[2]),
        pltpu.make_async_copy(f_in.at[0], f_own, in_sem.at[3]),
    ]
    for c in loads:
        c.start()

    barrier = pltpu.get_barrier_semaphore()

    def signal(where):
        pl.semaphore_signal(barrier, inc=1, device_id=where, device_id_type=MESH)

    def greet_cp(j, _):
        signal(cp_id(lax.rem(me + j, N_CP)))
        return 0

    def greet_quad(j, _):
        signal({"y": lax.rem(y + j, 4)})
        signal(row_id(lax.rem(x + j, 4)))
        return 0

    def greet_owner(zz, _):
        signal(owner_id(zz))
        return 0

    @pl.when(jnp.logical_not(stays))
    def _():
        lax.fori_loop(0, N_Z, greet_owner, 0)

    lax.fori_loop(1, N_CP, greet_cp, 0)
    lax.fori_loop(1, 4, greet_quad, 0)
    signal({"core": 1 - core})
    pl.semaphore_wait(barrier, jnp.where(stays, 22, 30))

    def far_first(i):
        return jnp.where(lax.rem(i, 2) == 0, 4 + i // 2, 3 - i // 2) % N_Z

    def head_at(i):
        return jnp.where(i < 2, N_Z + i, lax.rem(z + far_first(i - 2), N_Z))

    def cols_of(head):
        return pl.ds(pl.multiple_of(head * SPAN, SPAN), SPAN)

    ins = (k_in, q_in, g_in, v_in)
    bufs = (k_buf, q_buf, g_buf, v_buf)

    def source(t, head):
        return ins[t].at[0, :, cols_of(head)] if t < 4 else s_own.at[head]

    def target(t, block):
        return bufs[t].at[block] if t < 4 else s_buf.at[block]

    def send_all(kinds):
        def send(i, _):
            head = head_at(i)
            ox, oz = owner_of(head, core)

            @pl.when(head != mine)
            def _():
                for t in kinds:
                    pltpu.make_async_remote_copy(
                        src_ref=source(t, head), dst_ref=target(t, me),
                        send_sem=send_sem.at[t, head], recv_sem=recv_sem.at[t, me],
                        device_id={"x_lo": ox, "z": oz}, device_id_type=MESH).start()

            @pl.when(head == mine)
            def _():
                for t in kinds:
                    if t < 4:
                        pltpu.make_async_copy(source(t, head), target(t, me), recv_sem.at[t, me]).start()
                    else:
                        s_buf[me] = s_own[head]

            return 0

        lax.fori_loop(0, HEADS, send, 0)

    send_all((1, 2))

    for c in loads[:3]:
        c.wait()
    lse = l_own[...] * LOG2E
    s_own[...] = jnp.zeros_like(s_own)
    for h in range(HEADS):
        hs = slice(h * SPAN, (h + 1) * SPAN)
        product = g_own[:, hs].astype(F32) * o_own[:, hs].astype(F32)
        s_own[h, 0:1, :] = lse[h]
        s_own[h, 1:2, :] = jnp.sum(product.T, axis=0, keepdims=True)
    send_all((4,))
    send_all((0,))
    send_all((3,))

    loads[3].wait()

    def turn(i, _):
        at = pl.multiple_of(i * SPAN, SPAN)
        group = i // per
        rs = pl.ds(pl.multiple_of(lax.rem(i, per) * SPAN, SPAN), SPAN)
        ft_own[group // 2, lax.rem(group, 2), rs, :] = f_own[:, pl.ds(at, SPAN)].T
        return 0

    lax.fori_loop(0, feat // SPAN, turn, 0)
    my_rows = pl.ds(pl.multiple_of(y * SPAN, SPAN), SPAN)

    def feature_copy(j):
        to = lax.rem(y + j, 4)
        return pltpu.make_async_remote_copy(
            src_ref=ft_own.at[:, to // 2], dst_ref=ft_buf.at[:, :, my_rows],
            send_sem=f_ssem.at[j], recv_sem=f_rsem.at[j], device_id={"y": to},
            device_id_type=MESH)

    for j in range(1, 4):
        feature_copy(j).start()
    ft_buf[:, :, my_rows] = ft_own[:, y1]

    half_h = HEADS // 2

    def value_copy(h, o):
        to = h // half_h + 2 * o
        at = lax.rem(h, half_h)
        return to, pltpu.make_async_remote_copy(
            src_ref=back.at[0, :, cols_of(h)], dst_ref=dv_buf.at[my_rows, cols_of(at)],
            send_sem=y_ssem.at[h, o], recv_sem=y_rsem.at[y, at], device_id={"y": to},
            device_id_type=MESH)

    def pass_on(i, _):
        h = jnp.where(i < N_Z, lax.rem(z + far_first(i), N_Z), i)

        @pl.when(h != mine)
        def _():
            pltpu.make_async_copy(done.at[0, 0], back.at[0, :, cols_of(h)], ret_recv.at[0, h]).wait()

        for o in range(2):
            to, copy = value_copy(h, o)

            @pl.when(to != y)
            def _():
                copy.start()
        return 0

    UB = 2
    seq = N_CP * rows

    def block_at(i):
        return lax.rem(z + N_Z - far_first(i), N_Z)

    def arrive_pair(t, b):
        for xx in range(2):
            r = 2 * b + xx
            pltpu.make_async_copy(source(t, 0), target(t, r), recv_sem.at[t, r]).wait()

    def give(t, r):
        @pl.when(r != me)
        def _():
            pltpu.make_async_remote_copy(
                src_ref=done.at[t, r], dst_ref=back.at[t, :, cols_of(mine)],
                send_sem=ret_send.at[t, r], recv_sem=ret_recv.at[t, mine],
                device_id=cp_id(r), device_id_type=MESH).start()

        @pl.when(r == me)
        def _():
            back[t, :, cols_of(mine)] = done[t, me]

    @pl.when(active)
    def _():
        def arrive(kinds):
            def one(r, _):
                for t in kinds:
                    if t < 4:
                        pltpu.make_async_copy(source(t, 0), target(t, r), recv_sem.at[t, r]).wait()
                    else:
                        @pl.when(r != me)
                        def _():
                            pltpu.make_async_copy(source(t, 0), target(t, r), recv_sem.at[t, r]).wait()
                return 0
            lax.fori_loop(0, N_CP, one, 0)

        arrive((1, 2, 4))
        lse = jnp.concatenate([s_buf[i, 0:1, :] for i in range(N_CP)], axis=1)

        def value_step(i, _):
            b = block_at(i)
            us = pl.ds(b * UB, UB)
            arrive_pair(0, b)
            k = k_buf[us].reshape(UB * rows, SPAN)
            st = lax.dot_general(k, q_buf[...].reshape(seq, SPAN), NT, preferred_element_type=F32)
            p = jnp.exp2(st * (scale * LOG2E) - lse)
            prob[pl.ds(pl.multiple_of(b * UB * rows, UB * rows), UB * rows), :] = p
            dv = jnp.dot(p.astype(BF16), g_buf[...].reshape(seq, SPAN), preferred_element_type=F32)
            done[0, us] = dv.astype(BF16).reshape(UB, rows, SPAN)
            give(0, 2 * b)
            give(0, 2 * b + 1)
            return 0

        lax.fori_loop(0, N_CP // UB, value_step, 0)
        dq_acc[...] = jnp.zeros_like(dq_acc)


    def key_step(i):
        b = block_at(i)
        us = pl.ds(b * UB, UB)
        arrive_pair(3, b)
        k = k_buf[us].reshape(UB * rows, SPAN)
        v = v_buf[us].reshape(UB * rows, SPAN)
        delta = jnp.concatenate([s_buf[i, 1:2, :] for i in range(N_CP)], axis=1)
        p = prob[pl.ds(pl.multiple_of(b * UB * rows, UB * rows), UB * rows), :]
        dp = lax.dot_general(v, g_buf[...].reshape(seq, SPAN), NT, preferred_element_type=F32)
        ds = (p * (dp - delta)).astype(BF16)
        dk = jnp.dot(ds, q_buf[...].reshape(seq, SPAN), preferred_element_type=F32)
        done[1, us] = (dk * scale).astype(BF16).reshape(UB, rows, SPAN)
        dq_acc[...] += lax.dot_general(ds, k, TN, preferred_element_type=F32)
        give(1, 2 * b)
        give(1, 2 * b + 1)

    def key_or_pass(i, _):
        @pl.when(active)
        def _():
            key_step(i)

        pass_on(i, 0)
        return 0

    lax.fori_loop(0, N_Z, key_or_pass, 0)

    @pl.when(active)
    def _():
        done[2] = (dq_acc[...] * scale).astype(BF16).reshape(N_CP, rows, SPAN)

        def query_give(i, _):
            b = block_at(i)
            give(2, 2 * b)
            give(2, 2 * b + 1)
            return 0

        lax.fori_loop(0, N_Z, query_give, 0)

    outs = (dv_out, dk_out, dq_out)

    def collect_all(t):
        def collect(h, _):
            @pl.when(h != mine)
            def _():
                pltpu.make_async_copy(done.at[t, 0], back.at[t, :, cols_of(h)], ret_recv.at[t, h]).wait()
            return 0

        lax.fori_loop(0, HEADS, collect, 0)
        pltpu.make_async_copy(back.at[t], outs[t].at[0], out_sem.at[t]).start()

    lax.fori_loop(N_Z, HEADS, pass_on, 0)
    pltpu.make_async_copy(back.at[0], outs[0].at[0], out_sem.at[0]).start()
    dv_buf[my_rows, :] = back[0, :, pl.ds(pl.multiple_of(y0 * half_w, half_w), half_w)]
    for j in range(1, 4):
        feature_copy(j).wait()

    def values_from(i, _):
        from_y, at = lax.rem(y + 1 + i // half_h, 4), lax.rem(i, half_h)
        rs = pl.ds(pl.multiple_of(from_y * SPAN, SPAN), SPAN)
        pltpu.make_async_copy(
            back.at[0, :, cols_of(at)], dv_buf.at[rs, cols_of(at)], y_rsem.at[from_y, at]).wait()
        return 0

    lax.fori_loop(0, 3 * half_h, values_from, 0)

    def part_of(which, j):
        at = pl.multiple_of((lax.rem(j, 2) * 2 + which) * blk, blk)
        return jnp.dot(ft_buf[j // 2, pl.ds(at, blk), :], dv_buf[...], preferred_element_type=F32)

    def half_copy(j):
        return pltpu.make_async_remote_copy(
            src_ref=half_send.at[j], dst_ref=half_recv.at[j], send_sem=d_ssem.at[j],
            recv_sem=d_rsem.at[j], device_id={"core": 1 - core}, device_id_type=MESH)

    rows_x = blk // 2

    def x_copy(c, j):
        rs = pl.ds(c * rows_x, rows_x)
        return pltpu.make_async_remote_copy(
            src_ref=x_send.at[j, rs], dst_ref=x_recv.at[x, rs], send_sem=x_ssem.at[c, j],
            recv_sem=x_rsem.at[c, x], device_id=row_id(j), device_id_type=MESH)


    def to_other(o, _):
        j = lax.rem(x + 1 + o, 4)
        half_send[j] = part_of(1 - core, j).astype(BF16)
        half_copy(j).start()
        return 0

    def to_owner(o, _):
        j = lax.rem(x + 1 + o, 4)
        part[...] = part_of(core, j)
        half_copy(j).wait_recv()
        both = (part[...] + half_recv[j].astype(F32)).astype(BF16)

        @pl.when(j == x)
        def _():
            x_recv[x] = both

        @pl.when(j != x)
        def _():
            x_send[j] = both
            x_copy(0, j).start()
        return 0

    lax.fori_loop(0, 4, to_other, 0)
    lax.fori_loop(0, 4, to_owner, 0)
    for o in range(1, 4):
        x_copy(1, lax.rem(x + o, 4)).start()

    def z_copy(c, zz):
        return pltpu.make_async_remote_copy(
            src_ref=z_send.at[c, zz], dst_ref=z_recv.at[c, z], send_sem=z_ssem.at[c, zz],
            recv_sem=z_rsem.at[c, z], device_id=owner_id(zz), device_id_type=MESH)

    def is_here(zz):
        return jnp.logical_and(stays, zz == z)

    gap = jnp.zeros((rows_x, SPAN - col), BF16)
    for c in range(2):
        for o in range(1, 4):
            s = lax.rem(x + o, 4)
            rs = pl.ds(c * rows_x, rows_x)
            pltpu.make_async_copy(x_send.at[s, rs], x_recv.at[s, rs], x_rsem.at[c, s]).wait()
        both = x_recv[0, c * rows_x : (c + 1) * rows_x].astype(F32)
        for s in range(1, 4):
            both += x_recv[s, c * rows_x : (c + 1) * rows_x].astype(F32)
        for zz in range(N_Z):
            piece = both[:, zz * col : (zz + 1) * col].astype(BF16)
            z_send[c, zz] = jnp.concatenate([piece, gap], axis=1)

        def z_start(i, _):
            zz = lax.rem(z + far_first(i), N_Z)

            @pl.when(jnp.logical_not(is_here(zz)))
            def _():
                z_copy(c, zz).start()

            @pl.when(is_here(zz))
            def _():
                z_recv[c, zz] = z_send[c, zz]
            return 0

        lax.fori_loop(0, N_Z, z_start, 0)
    collect_all(1)
    collect_all(2)
    total[...] = jnp.zeros_like(total)
    for c in range(2):
        def z_take(i, _):
            zz = lax.rem(z + far_first(i), N_Z)

            @pl.when(jnp.logical_not(is_here(zz)))
            def _():
                pltpu.make_async_copy(
                    z_send.at[c, zz], z_recv.at[c, zz], z_rsem.at[c, zz]).wait()

            total[c * rows_x : (c + 1) * rows_x] += z_recv[c, zz][:, :col].astype(F32)
            return 0

        lax.fori_loop(0, N_Z, z_take, 0)
    last = pltpu.make_async_copy(total, dw_out, out_sem.at[3])
    last.start()

    def sent(head, _):
        @pl.when(head != mine)
        def _():
            for t in range(5):
                pltpu.make_async_copy(source(t, head), target(t, me), send_sem.at[t, head]).wait()
        return 0

    lax.fori_loop(0, HEADS, sent, 0)

    @pl.when(active)
    def _():
        def gave(j, _):
            peer = lax.rem(me + j, N_CP)
            for t in range(3):
                pltpu.make_async_copy(
                    done.at[t, peer], back.at[t, :, cols_of(mine)], ret_send.at[t, peer]).wait()
            return 0

        lax.fori_loop(1, N_CP, gave, 0)

    def passed(h, _):
        for o in range(2):
            to, copy = value_copy(h, o)

            @pl.when(to != y)
            def _():
                copy.wait_send()
        return 0

    lax.fori_loop(0, HEADS, passed, 0)

    def x_sent(j, _):
        half_copy(j).wait_send()

        @pl.when(j != x)
        def _():
            for c in range(2):
                x_copy(c, j).wait_send()
        return 0

    lax.fori_loop(0, 4, x_sent, 0)

    def z_sent(zz, _):
        @pl.when(jnp.logical_not(is_here(zz)))
        def _():
            for c in range(2):
                z_copy(c, zz).wait_send()
        return 0

    lax.fori_loop(0, N_Z, z_sent, 0)
    for t in range(3):
        pltpu.make_async_copy(back.at[t], outs[t].at[0], out_sem.at[t]).wait()
    last.wait()


def on_device(features, query_rows, key_rows, value_rows, attn_output, grad_output, log_sums):
    _, rows, width = query_rows.shape
    feat = features.shape[2]
    seq = N_CP * rows
    blk, half_w = feat // 16, width // 2
    any_spec = pl.BlockSpec(memory_space=pl.ANY)
    block = pltpu.VMEM((N_CP, rows, SPAN), BF16)
    out = jax.ShapeDtypeStruct(query_rows.shape, BF16)
    dma = pltpu.SemaphoreType.DMA
    return pl.pallas_call(
        functools.partial(step_kernel, scale=SPAN**-0.5, rows=rows),
        out_shape=(out, out, out, jax.ShapeDtypeStruct((blk, half_w // N_Z), F32)),
        in_specs=[any_spec] * 7,
        out_specs=(any_spec,) * 4,
        scratch_shapes=[
            block, block, block, block,
            pltpu.VMEM((N_CP, 8, rows), F32),
            pltpu.VMEM((seq, seq), F32),
            pltpu.VMEM((seq, SPAN), F32),
            pltpu.VMEM((3, N_CP, rows, SPAN), BF16),
            pltpu.VMEM((3, rows, width), BF16),
            pltpu.VMEM((rows, width), BF16),
            pltpu.VMEM((rows, width), BF16),
            pltpu.VMEM((HEADS, 1, rows), F32),
            pltpu.VMEM((HEADS, 8, rows), F32),
            pltpu.VMEM((rows, feat), BF16),
            pltpu.VMEM((2, 2, feat // 4, rows), BF16),
            pltpu.VMEM((2, feat // 4, 4 * rows), BF16),
            pltpu.VMEM((4 * rows, half_w), BF16),
            pltpu.VMEM((4, blk, half_w), BF16),
            pltpu.VMEM((4, blk, half_w), BF16),
            pltpu.VMEM((blk, half_w), F32),
            pltpu.VMEM((4, blk, half_w), BF16),
            pltpu.VMEM((4, blk, half_w), BF16),
            pltpu.VMEM((2, N_Z, blk // 2, SPAN), BF16),
            pltpu.VMEM((2, N_Z, blk // 2, SPAN), BF16),
            pltpu.VMEM((blk, half_w // N_Z), F32),
            dma((4,)),
            dma((5, HEADS)), dma((5, N_CP)), dma((3, N_CP)), dma((3, HEADS)), dma((4,)),
            dma((4,)), dma((4,)), dma((HEADS, 2)), dma((4, HEADS // 2)), dma((4,)), dma((4,)),
            dma((2, 4)), dma((2, 4)), dma((2, N_Z)), dma((2, N_Z)),
        ],
        compiler_params=pltpu.CompilerParams(
            collective_id=0, has_side_effects=True, vmem_limit_bytes=60 * 2**20),
        name="step",
    )(features, query_rows, key_rows, value_rows, attn_output, grad_output,
      jnp.transpose(log_sums, (2, 0, 1)))


def solution(mesh):
    finer = Mesh(mesh.devices.reshape(2, 4, 2, 2, 8), AXES)
    rows = P(FSDP, CP, None)
    return jax.shard_map(
        on_device, mesh=finer, in_specs=(rows,) * 7,
        out_specs=(rows, rows, rows, P(FSDP, CP)), check_vma=False,
    )
```

```python
import functools

import jax
import jax.numpy as jnp
from jax import lax
from jax.experimental import pallas as pl
from jax.experimental.pallas import tpu as pltpu
from jax.sharding import Mesh
from jax.sharding import PartitionSpec as P

AXES = ("x_hi", "y", "core", "x_lo", "z")
FSDP = ("x_hi", "y", "core")
CP = ("x_lo", "z")
LOG2E = 1.4426950408889634
HEADS = 10
HALF = HEADS // 2
SPAN = 128
N_CP = 16
N_Z = 8
MESH = pl.DeviceIdType.MESH
F32 = jnp.float32
BF16 = jnp.bfloat16
NT = (((1,), (1,)), ((), ()))
TN = (((0,), (0,)), ((), ()))


def owner_of(head, parity):
    spare = head >= N_Z
    z = jnp.where(spare, 2 * parity + 4 * (head - N_Z), head)
    x = jnp.where(spare, 1 - parity, lax.rem(head + parity, 2))
    return x, z


def head_of(x, z, parity):
    first = x == lax.rem(z + parity, 2)
    spare = jnp.where(z == 2 * parity, N_Z, jnp.where(z == 2 * parity + 4, N_Z + 1, HEADS))
    return jnp.where(first, z, spare)


def step_kernel(
    f_in, q_in, k_in, v_in, o_in, g_in, l_in, dq_out, dk_out, dv_out, dw_out,
    q_buf, k_buf, v_buf, g_buf, s_buf, prob, dq_acc, done, back,
    g_own, o_own, l_own, s_own, f_own, ft_own, ft_out, ft_buf, dv_buf,
    half_send, half_recv, part, x_send, x_recv, z_send, z_recv, total,
    in_sem, send_sem, recv_sem, ret_send, ret_recv, out_sem,
    f_ssem, f_rsem, y_ssem, y_rsem, d_ssem, d_rsem, x_ssem, x_rsem, z_ssem, z_rsem,
    *, scale, rows
):
    xh, y, core = lax.axis_index("x_hi"), lax.axis_index("y"), lax.axis_index("core")
    xl, z = lax.axis_index("x_lo"), lax.axis_index("z")
    x = 2 * xh + xl
    me = 2 * z + xl
    mine = head_of(xl, z, core)
    active = mine < HEADS
    feat = f_in.shape[2]
    half_w = q_in.shape[2] // 2
    blk = feat // 16
    piece = blk // 2
    col = half_w // N_Z

    def cp_id(peer):
        return {"x_lo": lax.rem(peer, 2), "z": peer // 2}

    def row_id(p):
        return {"x_hi": p // 2, "x_lo": lax.rem(p, 2)}

    def y_id(p):
        return {"y": p}

    near, near_id = (y, x), (y_id, row_id)
    across, across_id = (x, y), (row_id, y_id)

    loads = [
        pltpu.make_async_copy(g_in.at[0], g_own, in_sem.at[0]),
        pltpu.make_async_copy(o_in.at[0], o_own, in_sem.at[1]),
        pltpu.make_async_copy(l_in, l_own, in_sem.at[2]),
        pltpu.make_async_copy(f_in.at[0], f_own, in_sem.at[3]),
    ]
    for c in loads:
        c.start()

    barrier = pltpu.get_barrier_semaphore()

    def signal(where):
        pl.semaphore_signal(barrier, inc=1, device_id=where, device_id_type=MESH)

    def greet_cp(j, _):
        signal(cp_id(lax.rem(me + j, N_CP)))
        return 0

    def greet_quad(j, _):
        signal({"y": lax.rem(y + j, 4)})
        signal(row_id(lax.rem(x + j, 4)))
        return 0

    lax.fori_loop(1, N_CP, greet_cp, 0)
    lax.fori_loop(1, 4, greet_quad, 0)
    signal({"core": 1 - core})
    pl.semaphore_wait(barrier, N_CP + 6)

    def far_first(i):
        return jnp.where(lax.rem(i, 2) == 0, 4 + i // 2, 3 - i // 2) % N_Z

    def head_at(i):
        return jnp.where(i < 2, N_Z + i, lax.rem(z + far_first(i - 2), N_Z))

    def cols_of(head):
        return pl.ds(pl.multiple_of(head * SPAN, SPAN), SPAN)

    ins = (k_in, q_in, g_in, v_in)
    bufs = (k_buf, q_buf, g_buf, v_buf)

    def source(t, head):
        return ins[t].at[0, :, cols_of(head)] if t < 4 else s_own.at[head]

    def target(t, block):
        return bufs[t].at[block] if t < 4 else s_buf.at[block]

    def send_all(kinds):
        def send(i, _):
            head = head_at(i)
            ox, oz = owner_of(head, core)

            @pl.when(head != mine)
            def _():
                for t in kinds:
                    pltpu.make_async_remote_copy(
                        src_ref=source(t, head), dst_ref=target(t, me),
                        send_sem=send_sem.at[t, head], recv_sem=recv_sem.at[t, me],
                        device_id={"x_lo": ox, "z": oz}, device_id_type=MESH).start()

            @pl.when(head == mine)
            def _():
                for t in kinds:
                    if t < 4:
                        pltpu.make_async_copy(source(t, head), target(t, me), recv_sem.at[t, me]).start()
                    else:
                        s_buf[me] = s_own[head]

            return 0

        lax.fori_loop(0, HEADS, send, 0)

    send_all((1, 2))

    for c in loads[:3]:
        c.wait()
    lse = l_own[...] * LOG2E
    s_own[...] = jnp.zeros_like(s_own)
    for h in range(HEADS):
        hs = slice(h * SPAN, (h + 1) * SPAN)
        product = g_own[:, hs].astype(F32) * o_own[:, hs].astype(F32)
        s_own[h, 0:1, :] = lse[h]
        s_own[h, 1:2, :] = jnp.sum(product.T, axis=0, keepdims=True)
    send_all((4,))
    send_all((0,))

    loads[3].wait()

    def turn(i, _):
        at = pl.multiple_of(i * SPAN, SPAN)
        ft_own[pl.ds(at, SPAN), :] = f_own[:, pl.ds(at, SPAN)].T
        return 0

    lax.fori_loop(0, feat // SPAN, turn, 0)

    def sort(i, _):
        f, part_s = i // 2, lax.rem(i, 2)
        of_y, of_x, of_core = lax.rem(f // 2, 4), 2 * (f // 8) + part_s, lax.rem(f, 2)
        value = ft_own[pl.ds(pl.multiple_of(i * piece, piece), piece), :]
        ft_out[0, of_y, pl.ds(pl.multiple_of((of_core * 4 + of_x) * piece, piece), piece), :] = value
        ft_out[1, of_x, pl.ds(pl.multiple_of((of_core * 4 + of_y) * piece, piece), piece), :] = value
        return 0

    lax.fori_loop(0, feat // piece, sort, 0)

    def my_span(w):
        return pl.ds(pl.multiple_of(near[w] * SPAN, SPAN), SPAN)

    def feature_copy(w, j):
        to = lax.rem(near[w] + j, 4)
        return pltpu.make_async_remote_copy(
            src_ref=ft_out.at[w, to], dst_ref=ft_buf.at[w, :, my_span(w)],
            send_sem=f_ssem.at[w, j], recv_sem=f_rsem.at[w, j], device_id=near_id[w](to),
            device_id_type=MESH)

    for w in range(2):
        for j in range(1, 4):
            feature_copy(w, j).start()
        ft_buf[w, :, my_span(w)] = ft_out[w, near[w]]

    def left(kinds):
        def one(head, _):
            @pl.when(head != mine)
            def _():
                for t in kinds:
                    pltpu.make_async_copy(source(t, head), target(t, me), send_sem.at[t, head]).wait()
            return 0

        lax.fori_loop(0, HEADS, one, 0)

    left((1, 2))
    left((0,))
    send_all((3,))

    def value_copy(w, h, o):
        return pltpu.make_async_remote_copy(
            src_ref=back.at[0, :, cols_of(h)],
            dst_ref=dv_buf.at[w, my_span(w), cols_of(h - HALF * w)],
            send_sem=y_ssem.at[h, o], recv_sem=y_rsem.at[near[w], h],
            device_id=near_id[w](lax.rem(near[w] + o, 4)), device_id_type=MESH)

    def pass_on(i, _):
        h = jnp.where(i < N_Z, lax.rem(z + far_first(i), N_Z), i)

        @pl.when(h != mine)
        def _():
            pltpu.make_async_copy(done.at[0, 0], back.at[0, :, cols_of(h)], ret_recv.at[0, h]).wait()

        for w in range(2):
            @pl.when(h // HALF == w)
            def _():
                for o in range(1, 4):
                    value_copy(w, h, o).start()
        return 0

    UB = 2
    seq = N_CP * rows

    def block_at(i):
        return lax.rem(z + N_Z - far_first(i), N_Z)

    def arrive_pair(t, b):
        for xx in range(2):
            r = 2 * b + xx
            pltpu.make_async_copy(source(t, 0), target(t, r), recv_sem.at[t, r]).wait()

    def give(t, r):
        @pl.when(r != me)
        def _():
            pltpu.make_async_remote_copy(
                src_ref=done.at[t, r], dst_ref=back.at[t, :, cols_of(mine)],
                send_sem=ret_send.at[t, r], recv_sem=ret_recv.at[t, mine],
                device_id=cp_id(r), device_id_type=MESH).start()

        @pl.when(r == me)
        def _():
            back[t, :, cols_of(mine)] = done[t, me]

    @pl.when(active)
    def _():
        def arrive(kinds):
            def one(r, _):
                for t in kinds:
                    if t < 4:
                        pltpu.make_async_copy(source(t, 0), target(t, r), recv_sem.at[t, r]).wait()
                    else:
                        @pl.when(r != me)
                        def _():
                            pltpu.make_async_copy(source(t, 0), target(t, r), recv_sem.at[t, r]).wait()
                return 0
            lax.fori_loop(0, N_CP, one, 0)

        arrive((1, 2, 4))
        lse = jnp.concatenate([s_buf[i, 0:1, :] for i in range(N_CP)], axis=1)

        def value_step(i, _):
            b = block_at(i)
            us = pl.ds(b * UB, UB)
            arrive_pair(0, b)
            k = k_buf[us].reshape(UB * rows, SPAN)
            st = lax.dot_general(k, q_buf[...].reshape(seq, SPAN), NT, preferred_element_type=F32)
            p = jnp.exp2(st * (scale * LOG2E) - lse)
            prob[pl.ds(pl.multiple_of(b * UB * rows, UB * rows), UB * rows), :] = p
            dv = jnp.dot(p.astype(BF16), g_buf[...].reshape(seq, SPAN), preferred_element_type=F32)
            done[0, us] = dv.astype(BF16).reshape(UB, rows, SPAN)
            give(0, 2 * b)
            give(0, 2 * b + 1)
            return 0

        lax.fori_loop(0, N_CP // UB, value_step, 0)
        dq_acc[...] = jnp.zeros_like(dq_acc)


    def key_step(i):
        b = block_at(i)
        us = pl.ds(b * UB, UB)
        arrive_pair(3, b)
        k = k_buf[us].reshape(UB * rows, SPAN)
        v = v_buf[us].reshape(UB * rows, SPAN)
        delta = jnp.concatenate([s_buf[i, 1:2, :] for i in range(N_CP)], axis=1)
        p = prob[pl.ds(pl.multiple_of(b * UB * rows, UB * rows), UB * rows), :]
        dp = lax.dot_general(v, g_buf[...].reshape(seq, SPAN), NT, preferred_element_type=F32)
        ds = (p * (dp - delta)).astype(BF16)
        dk = jnp.dot(ds, q_buf[...].reshape(seq, SPAN), preferred_element_type=F32)
        done[1, us] = (dk * scale).astype(BF16).reshape(UB, rows, SPAN)
        dq_acc[...] += lax.dot_general(ds, k, TN, preferred_element_type=F32)
        give(1, 2 * b)
        give(1, 2 * b + 1)

    def key_steps(lo, hi):
        def one(i, _):
            @pl.when(active)
            def _():
                key_step(i)
            return 0

        lax.fori_loop(lo, hi, one, 0)

    def finish_queries():
        done[2] = (dq_acc[...] * scale).astype(BF16).reshape(N_CP, rows, SPAN)

        def query_give(i, _):
            b = block_at(i)
            give(2, 2 * b)
            give(2, 2 * b + 1)
            return 0

        lax.fori_loop(0, N_Z, query_give, 0)

    def passes(lo, hi):
        lax.fori_loop(lo, hi, pass_on, 0)

    passes(0, HEADS)
    key_steps(0, N_Z)
    pl.when(active)(finish_queries)

    outs = (dv_out, dk_out, dq_out)

    def collect_all(t):
        def collect(h, _):
            @pl.when(h != mine)
            def _():
                pltpu.make_async_copy(done.at[t, 0], back.at[t, :, cols_of(h)], ret_recv.at[t, h]).wait()
            return 0

        lax.fori_loop(0, HEADS, collect, 0)
        pltpu.make_async_copy(back.at[t], outs[t].at[0], out_sem.at[t]).start()

    pltpu.make_async_copy(back.at[0], outs[0].at[0], out_sem.at[0]).start()

    for w in range(2):
        dv_buf[w, my_span(w), :] = back[0, :, w * half_w : (w + 1) * half_w]
    for w in range(2):
        for j in range(1, 4):
            feature_copy(w, j).wait()

    def values_from(w):
        def one(i, _):
            source_at, at = lax.rem(near[w] + 1 + i // HALF, 4), lax.rem(i, HALF)
            rs = pl.ds(pl.multiple_of(source_at * SPAN, SPAN), SPAN)
            pltpu.make_async_copy(
                back.at[0, :, cols_of(at)], dv_buf.at[w, rs, cols_of(at)],
                y_rsem.at[source_at, HALF * w + at]).wait()
            return 0

        lax.fori_loop(0, 3 * HALF, one, 0)

    def part_of(w, which):
        rs = pl.ds(pl.multiple_of(which * 2 * blk, 2 * blk), 2 * blk)
        return jnp.dot(ft_buf[w, rs, :], dv_buf[w], preferred_element_type=F32)

    def half_copy(w):
        return pltpu.make_async_remote_copy(
            src_ref=half_send.at[w], dst_ref=half_recv.at[w], send_sem=d_ssem.at[w],
            recv_sem=d_rsem.at[w], device_id={"core": 1 - core}, device_id_type=MESH)

    def across_copy(w, j):
        return pltpu.make_async_remote_copy(
            src_ref=x_send.at[w, j], dst_ref=x_recv.at[w, across[w]], send_sem=x_ssem.at[w, j],
            recv_sem=x_rsem.at[w, across[w]], device_id=across_id[w](j), device_id_type=MESH)

    for w in range(2):
        values_from(w)
        half_send[w] = part_of(w, 1 - core).astype(BF16)
        half_copy(w).start()
    for w in range(2):
        part[...] = part_of(w, core)
        half_copy(w).wait_recv()
        both = (part[...] + half_recv[w].astype(F32)).astype(BF16)
        x_send[w] = both.reshape(4, piece, half_w)
        for o in range(1, 4):
            across_copy(w, lax.rem(across[w] + o, 4)).start()
        x_recv[w, across[w]] = x_send[w, across[w]]

    def z_copy(w, zz):
        return pltpu.make_async_remote_copy(
            src_ref=z_send.at[w, zz], dst_ref=z_recv.at[xl, z], send_sem=z_ssem.at[w, zz],
            recv_sem=z_rsem.at[xl, z], device_id={"x_lo": w, "z": zz}, device_id_type=MESH)

    def is_here(w, zz):
        return jnp.logical_and(xl == w, zz == z)

    gap = jnp.zeros((piece, SPAN - col), BF16)
    for w in range(2):
        for o in range(1, 4):
            s = lax.rem(across[w] + o, 4)
            pltpu.make_async_copy(x_send.at[w, s], x_recv.at[w, s], x_rsem.at[w, s]).wait()
        both = x_recv[w, 0].astype(F32)
        for s in range(1, 4):
            both += x_recv[w, s].astype(F32)
        for zz in range(N_Z):
            block16 = both[:, zz * col : (zz + 1) * col].astype(BF16)
            z_send[w, zz] = jnp.concatenate([block16, gap], axis=1)

        def z_start(i, _):
            zz = lax.rem(z + far_first(i), N_Z)

            @pl.when(jnp.logical_not(is_here(w, zz)))
            def _():
                z_copy(w, zz).start()

            @pl.when(is_here(w, zz))
            def _():
                z_recv[xl, zz] = z_send[w, zz]
            return 0

        lax.fori_loop(0, N_Z, z_start, 0)

    collect_all(1)
    collect_all(2)
    left((4, 3))
    @pl.when(active)
    def _():
        def gave(j, _):
            peer = lax.rem(me + j, N_CP)
            for t in range(3):
                pltpu.make_async_copy(
                    done.at[t, peer], back.at[t, :, cols_of(mine)], ret_send.at[t, peer]).wait()
            return 0

        lax.fori_loop(1, N_CP, gave, 0)

    def passed(h, _):
        for w in range(2):
            @pl.when(h // HALF == w)
            def _():
                for o in range(1, 4):
                    value_copy(w, h, o).wait_send()
        return 0

    lax.fori_loop(0, HEADS, passed, 0)
    for w in range(2):
        half_copy(w).wait_send()
        for o in range(1, 4):
            across_copy(w, lax.rem(across[w] + o, 4)).wait_send()

    total[...] = jnp.zeros_like(total)
    for xs in range(2):
        def take(i, _):
            zz = lax.rem(z + far_first(i), N_Z)

            @pl.when(jnp.logical_not(jnp.logical_and(xl == xs, zz == z)))
            def _():
                pltpu.make_async_copy(z_send.at[0, zz], z_recv.at[xs, zz], z_rsem.at[xs, zz]).wait()

            total[xs * piece : (xs + 1) * piece] += z_recv[xs, zz][:, :col].astype(F32)
            return 0

        lax.fori_loop(0, N_Z, take, 0)
    last = pltpu.make_async_copy(total, dw_out, out_sem.at[3])
    last.start()

    def z_sent(zz, _):
        for w in range(2):
            @pl.when(jnp.logical_not(is_here(w, zz)))
            def _():
                z_copy(w, zz).wait_send()
        return 0

    lax.fori_loop(0, N_Z, z_sent, 0)
    for t in range(3):
        pltpu.make_async_copy(back.at[t], outs[t].at[0], out_sem.at[t]).wait()
    last.wait()


def on_device(features, query_rows, key_rows, value_rows, attn_output, grad_output, log_sums):
    _, rows, width = query_rows.shape
    feat = features.shape[2]
    seq = N_CP * rows
    blk, half_w = feat // 16, width // 2
    any_spec = pl.BlockSpec(memory_space=pl.ANY)
    block = pltpu.VMEM((N_CP, rows, SPAN), BF16)
    out = jax.ShapeDtypeStruct(query_rows.shape, BF16)
    dma = pltpu.SemaphoreType.DMA
    return pl.pallas_call(
        functools.partial(step_kernel, scale=SPAN**-0.5, rows=rows),
        out_shape=(out, out, out, jax.ShapeDtypeStruct((blk, half_w // N_Z), F32)),
        in_specs=[any_spec] * 7,
        out_specs=(any_spec,) * 4,
        scratch_shapes=[
            block, block, block, block,
            pltpu.VMEM((N_CP, 8, rows), F32),
            pltpu.VMEM((seq, seq), F32),
            pltpu.VMEM((seq, SPAN), F32),
            pltpu.VMEM((3, N_CP, rows, SPAN), BF16),
            pltpu.VMEM((3, rows, width), BF16),
            pltpu.VMEM((rows, width), BF16),
            pltpu.VMEM((rows, width), BF16),
            pltpu.VMEM((HEADS, 1, rows), F32),
            pltpu.VMEM((HEADS, 8, rows), F32),
            pltpu.VMEM((rows, feat), BF16),
            pltpu.VMEM((feat, rows), BF16),
            pltpu.VMEM((2, 4, feat // 4, rows), BF16),
            pltpu.VMEM((2, feat // 4, 4 * rows), BF16),
            pltpu.VMEM((2, 4 * rows, half_w), BF16),
            pltpu.VMEM((2, 2 * blk, half_w), BF16),
            pltpu.VMEM((2, 2 * blk, half_w), BF16),
            pltpu.VMEM((2 * blk, half_w), F32),
            pltpu.VMEM((2, 4, blk // 2, half_w), BF16),
            pltpu.VMEM((2, 4, blk // 2, half_w), BF16),
            pltpu.VMEM((2, N_Z, blk // 2, SPAN), BF16),
            pltpu.VMEM((2, N_Z, blk // 2, SPAN), BF16),
            pltpu.VMEM((blk, half_w // N_Z), F32),
            dma((4,)),
            dma((5, HEADS)), dma((5, N_CP)), dma((3, N_CP)), dma((3, HEADS)), dma((4,)),
            dma((2, 4)), dma((2, 4)), dma((HEADS, 4)), dma((4, HEADS)), dma((2,)), dma((2,)),
            dma((2, 4)), dma((2, 4)), dma((2, N_Z)), dma((2, N_Z)),
        ],
        compiler_params=pltpu.CompilerParams(
            collective_id=0, has_side_effects=True, vmem_limit_bytes=60 * 2**20),
        name="step",
    )(features, query_rows, key_rows, value_rows, attn_output, grad_output,
      jnp.transpose(log_sums, (2, 0, 1)))


def solution(mesh):
    finer = Mesh(mesh.devices.reshape(2, 4, 2, 2, 8), AXES)
    rows = P(FSDP, CP, None)
    return jax.shard_map(
        on_device, mesh=finer, in_specs=(rows,) * 7,
        out_specs=(rows, rows, rows, P(FSDP, CP)), check_vma=False,
    )
```

```python
import functools

import jax
import jax.numpy as jnp
from jax import lax
from jax.experimental import pallas as pl
from jax.experimental.pallas import tpu as pltpu
from jax.sharding import Mesh
from jax.sharding import PartitionSpec as P

AXES = ("x_hi", "y", "core", "x_lo", "z")
FSDP = ("x_hi", "y", "core")
CP = ("x_lo", "z")
LOG2E = 1.4426950408889634
HEADS = 10
HALF = HEADS // 2
SPAN = 128
N_CP = 16
N_Z = 8
MESH = pl.DeviceIdType.MESH
F32 = jnp.float32
BF16 = jnp.bfloat16
NT = (((1,), (1,)), ((), ()))
TN = (((0,), (0,)), ((), ()))


def owner_of(head, parity):
    spare = head >= N_Z
    z = jnp.where(spare, 2 * parity + 4 * (head - N_Z), head)
    x = jnp.where(spare, 1 - parity, lax.rem(head + parity, 2))
    return x, z


def head_of(x, z, parity):
    first = x == lax.rem(z + parity, 2)
    spare = jnp.where(z == 2 * parity, N_Z, jnp.where(z == 2 * parity + 4, N_Z + 1, HEADS))
    return jnp.where(first, z, spare)


def step_kernel(
    f_in, q_in, k_in, v_in, o_in, g_in, l_in, dq_out, dk_out, dv_out, dw_out,
    q_buf, k_buf, v_buf, g_buf, s_buf, prob, dq_acc, done, back,
    g_own, o_own, l_own, s_own, f_own, ft_own, ft_out, ft_buf, dv_buf,
    half_send, half_recv, part, x_send, x_recv, z_send, z_recv, total,
    in_sem, send_sem, recv_sem, pair_sem, ret_send, ret_recv, value_sem, out_sem,
    f_ssem, f_rsem, y_ssem, y_rsem, d_ssem, d_rsem, x_ssem, x_rsem, z_ssem, z_rsem,
    *, scale, rows
):
    xh, y, core = lax.axis_index("x_hi"), lax.axis_index("y"), lax.axis_index("core")
    xl, z = lax.axis_index("x_lo"), lax.axis_index("z")
    x = 2 * xh + xl
    me = 2 * z + xl
    mine = head_of(xl, z, core)
    active = mine < HEADS
    feat = f_in.shape[2]
    half_w = q_in.shape[2] // 2
    blk = feat // 16
    piece = blk // 2
    col = half_w // N_Z

    def cp_id(peer):
        return {"x_lo": lax.rem(peer, 2), "z": peer // 2}

    def row_id(p):
        return {"x_hi": p // 2, "x_lo": lax.rem(p, 2)}

    def y_id(p):
        return {"y": p}

    near, near_id = (y, x), (y_id, row_id)
    across, across_id = (x, y), (row_id, y_id)

    loads = [
        pltpu.make_async_copy(g_in.at[0], g_own, in_sem.at[0]),
        pltpu.make_async_copy(o_in.at[0], o_own, in_sem.at[1]),
        pltpu.make_async_copy(l_in, l_own, in_sem.at[2]),
        pltpu.make_async_copy(f_in.at[0], f_own, in_sem.at[3]),
    ]
    for c in loads:
        c.start()

    barrier = pltpu.get_barrier_semaphore()

    def signal(where):
        pl.semaphore_signal(barrier, inc=1, device_id=where, device_id_type=MESH)

    def greet_cp(j, _):
        signal(cp_id(lax.rem(me + j, N_CP)))
        return 0

    def greet_quad(j, _):
        signal({"y": lax.rem(y + j, 4)})
        signal(row_id(lax.rem(x + j, 4)))
        return 0

    lax.fori_loop(1, N_CP, greet_cp, 0)
    lax.fori_loop(1, 4, greet_quad, 0)
    signal({"core": 1 - core})
    pl.semaphore_wait(barrier, N_CP + 6)

    def far_first(i):
        return jnp.where(lax.rem(i, 2) == 0, 4 + i // 2, 3 - i // 2) % N_Z

    def head_at(i):
        return jnp.where(i < 2, N_Z + i, lax.rem(z + far_first(i - 2), N_Z))

    def cols_of(head):
        return pl.ds(pl.multiple_of(head * SPAN, SPAN), SPAN)

    ins = (k_in, q_in, g_in, v_in)
    bufs = (k_buf, q_buf, g_buf, v_buf)

    def source(t, head):
        return ins[t].at[0, :, cols_of(head)] if t < 4 else s_own.at[head]

    def target(t, block):
        return bufs[t].at[block] if t < 4 else s_buf.at[block]

    def landed(t, b):
        return pair_sem.at[0 if t == 0 else 1, b] if t in (0, 3) else recv_sem.at[t]

    def send_all(kinds):
        def send(i, _):
            head = head_at(i)
            ox, oz = owner_of(head, core)

            @pl.when(head != mine)
            def _():
                for t in kinds:
                    pltpu.make_async_remote_copy(
                        src_ref=source(t, head), dst_ref=target(t, me),
                        send_sem=send_sem.at[t], recv_sem=landed(t, z),
                        device_id={"x_lo": ox, "z": oz}, device_id_type=MESH).start()

            @pl.when(head == mine)
            def _():
                for t in kinds:
                    if t < 4:
                        pltpu.make_async_copy(source(t, head), target(t, me), landed(t, z)).start()
                    else:
                        s_buf[me] = s_own[head]

            return 0

        lax.fori_loop(0, HEADS, send, 0)

    send_all((1, 2))

    for c in loads[:3]:
        c.wait()
    lse = l_own[...] * LOG2E
    s_own[...] = jnp.zeros_like(s_own)
    for h in range(HEADS):
        hs = slice(h * SPAN, (h + 1) * SPAN)
        product = g_own[:, hs].astype(F32) * o_own[:, hs].astype(F32)
        s_own[h, 0:1, :] = lse[h]
        s_own[h, 1:2, :] = jnp.sum(product.T, axis=0, keepdims=True)
    send_all((4,))
    send_all((0,))

    loads[3].wait()

    def turn(i, _):
        at = pl.multiple_of(i * SPAN, SPAN)
        ft_own[pl.ds(at, SPAN), :] = f_own[:, pl.ds(at, SPAN)].T
        return 0

    lax.fori_loop(0, feat // SPAN, turn, 0)

    def sort(i, _):
        f, part_s = i // 2, lax.rem(i, 2)
        of_y, of_x, of_core = lax.rem(f // 2, 4), 2 * (f // 8) + part_s, lax.rem(f, 2)
        value = ft_own[pl.ds(pl.multiple_of(i * piece, piece), piece), :]
        ft_out[0, of_y, pl.ds(pl.multiple_of((of_core * 4 + of_x) * piece, piece), piece), :] = value
        ft_out[1, of_x, pl.ds(pl.multiple_of((of_core * 4 + of_y) * piece, piece), piece), :] = value
        return 0

    lax.fori_loop(0, feat // piece, sort, 0)

    def my_span(w):
        return pl.ds(pl.multiple_of(near[w] * SPAN, SPAN), SPAN)

    def feature_copy(w, j):
        to = lax.rem(near[w] + j, 4)
        return pltpu.make_async_remote_copy(
            src_ref=ft_out.at[w, to], dst_ref=ft_buf.at[w, :, my_span(w)],
            send_sem=f_ssem.at[w, j], recv_sem=f_rsem.at[w, j], device_id=near_id[w](to),
            device_id_type=MESH)

    for w in range(2):
        for j in range(1, 4):
            feature_copy(w, j).start()
        ft_buf[w, :, my_span(w)] = ft_out[w, near[w]]

    def gone(ref, sem):
        pltpu.make_async_copy(ref, ref, sem).wait()

    def left(kinds):
        def count(n):
            for t in kinds:
                gone(ins[t].at[0, :, : n * SPAN] if t < 4 else s_own.at[:n], send_sem.at[t])

        pl.when(active)(lambda: count(HEADS - 1))
        pl.when(jnp.logical_not(active))(lambda: count(HEADS))

    left((1, 2))
    left((0,))
    send_all((3,))

    def value_copy(w, h, o):
        return pltpu.make_async_remote_copy(
            src_ref=back.at[0, :, cols_of(h)],
            dst_ref=dv_buf.at[w, my_span(w), cols_of(h - HALF * w)],
            send_sem=y_ssem.at[0], recv_sem=y_rsem.at[w, near[w]],
            device_id=near_id[w](lax.rem(near[w] + o, 4)), device_id_type=MESH)

    def pass_on(i, _):
        h = jnp.where(i < N_Z, lax.rem(z + far_first(i), N_Z), i)

        @pl.when(h != mine)
        def _():
            gone(back.at[0, :, cols_of(h)], value_sem.at[h])

        for w in range(2):
            @pl.when(h // HALF == w)
            def _():
                for o in range(1, 4):
                    value_copy(w, h, o).start()
        return 0

    UB = 2
    seq = N_CP * rows

    def block_at(i):
        return lax.rem(z + N_Z - far_first(i), N_Z)

    def arrive_pair(t, b):
        gone(bufs[t].at[pl.ds(2 * b, 2)], landed(t, b))

    def give(t, r):
        @pl.when(r != me)
        def _():
            pltpu.make_async_remote_copy(
                src_ref=done.at[t, r], dst_ref=back.at[t, :, cols_of(mine)],
                send_sem=ret_send.at[t], recv_sem=value_sem.at[mine] if t == 0 else ret_recv.at[t],
                device_id=cp_id(r), device_id_type=MESH).start()

        @pl.when(r == me)
        def _():
            back[t, :, cols_of(mine)] = done[t, me]

    @pl.when(active)
    def _():
        gone(q_buf, recv_sem.at[1])
        gone(g_buf, recv_sem.at[2])
        gone(s_buf.at[: N_CP - 1], recv_sem.at[4])
        lse = jnp.concatenate([s_buf[i, 0:1, :] for i in range(N_CP)], axis=1)

        def value_step(i, _):
            b = block_at(i)
            us = pl.ds(b * UB, UB)
            arrive_pair(0, b)
            k = k_buf[us].reshape(UB * rows, SPAN)
            st = lax.dot_general(k, q_buf[...].reshape(seq, SPAN), NT, preferred_element_type=F32)
            p = jnp.exp2(st * (scale * LOG2E) - lse)
            prob[pl.ds(pl.multiple_of(b * UB * rows, UB * rows), UB * rows), :] = p
            dv = jnp.dot(p.astype(BF16), g_buf[...].reshape(seq, SPAN), preferred_element_type=F32)
            done[0, us] = dv.astype(BF16).reshape(UB, rows, SPAN)
            give(0, 2 * b)
            give(0, 2 * b + 1)
            return 0

        lax.fori_loop(0, N_CP // UB, value_step, 0)
        dq_acc[...] = jnp.zeros_like(dq_acc)


    def key_step(i):
        b = block_at(i)
        us = pl.ds(b * UB, UB)
        arrive_pair(3, b)
        k = k_buf[us].reshape(UB * rows, SPAN)
        v = v_buf[us].reshape(UB * rows, SPAN)
        delta = jnp.concatenate([s_buf[i, 1:2, :] for i in range(N_CP)], axis=1)
        p = prob[pl.ds(pl.multiple_of(b * UB * rows, UB * rows), UB * rows), :]
        dp = lax.dot_general(v, g_buf[...].reshape(seq, SPAN), NT, preferred_element_type=F32)
        ds = (p * (dp - delta)).astype(BF16)
        dk = jnp.dot(ds, q_buf[...].reshape(seq, SPAN), preferred_element_type=F32)
        done[1, us] = (dk * scale).astype(BF16).reshape(UB, rows, SPAN)
        dq_acc[...] += lax.dot_general(ds, k, TN, preferred_element_type=F32)
        give(1, 2 * b)
        give(1, 2 * b + 1)

    def key_steps(lo, hi):
        def one(i, _):
            @pl.when(active)
            def _():
                key_step(i)
            return 0

        lax.fori_loop(lo, hi, one, 0)

    def finish_queries():
        done[2] = (dq_acc[...] * scale).astype(BF16).reshape(N_CP, rows, SPAN)

        def query_give(i, _):
            b = block_at(i)
            give(2, 2 * b)
            give(2, 2 * b + 1)
            return 0

        lax.fori_loop(0, N_Z, query_give, 0)

    def passes(lo, hi):
        lax.fori_loop(lo, hi, pass_on, 0)

    passes(0, HEADS)
    key_steps(0, N_Z)
    pl.when(active)(finish_queries)

    outs = (dv_out, dk_out, dq_out)

    def collect_all(t):
        pl.when(active)(lambda: gone(back.at[t, :, : (HEADS - 1) * SPAN], ret_recv.at[t]))
        pl.when(jnp.logical_not(active))(lambda: gone(back.at[t], ret_recv.at[t]))
        pltpu.make_async_copy(back.at[t], outs[t].at[0], out_sem.at[t]).start()

    pltpu.make_async_copy(back.at[0], outs[0].at[0], out_sem.at[0]).start()

    for w in range(2):
        dv_buf[w, my_span(w), :] = back[0, :, w * half_w : (w + 1) * half_w]
    for w in range(2):
        for j in range(1, 4):
            feature_copy(w, j).wait()

    def values_from(w):
        for o in range(1, 4):
            peer = lax.rem(near[w] + o, 4)
            gone(dv_buf.at[w, pl.ds(pl.multiple_of(peer * SPAN, SPAN), SPAN), :], y_rsem.at[w, peer])

    def part_of(w, which):
        rs = pl.ds(pl.multiple_of(which * 2 * blk, 2 * blk), 2 * blk)
        return jnp.dot(ft_buf[w, rs, :], dv_buf[w], preferred_element_type=F32)

    def half_copy(w):
        return pltpu.make_async_remote_copy(
            src_ref=half_send.at[w], dst_ref=half_recv.at[w], send_sem=d_ssem.at[w],
            recv_sem=d_rsem.at[w], device_id={"core": 1 - core}, device_id_type=MESH)

    def across_copy(w, j):
        return pltpu.make_async_remote_copy(
            src_ref=x_send.at[w, j], dst_ref=x_recv.at[w, across[w]], send_sem=x_ssem.at[w, j],
            recv_sem=x_rsem.at[w, across[w]], device_id=across_id[w](j), device_id_type=MESH)

    for w in range(2):
        values_from(w)
        half_send[w] = part_of(w, 1 - core).astype(BF16)
        half_copy(w).start()
    for w in range(2):
        part[...] = part_of(w, core)
        half_copy(w).wait_recv()
        both = (part[...] + half_recv[w].astype(F32)).astype(BF16)
        x_send[w] = both.reshape(4, piece, half_w)
        for o in range(1, 4):
            across_copy(w, lax.rem(across[w] + o, 4)).start()
        x_recv[w, across[w]] = x_send[w, across[w]]

    def z_copy(w, zz):
        return pltpu.make_async_remote_copy(
            src_ref=z_send.at[w, zz], dst_ref=z_recv.at[xl, z], send_sem=z_ssem.at[w],
            recv_sem=z_rsem.at[xl], device_id={"x_lo": w, "z": zz}, device_id_type=MESH)

    def is_here(w, zz):
        return jnp.logical_and(xl == w, zz == z)

    gap = jnp.zeros((piece, SPAN - col), BF16)
    for w in range(2):
        for o in range(1, 4):
            s = lax.rem(across[w] + o, 4)
            pltpu.make_async_copy(x_send.at[w, s], x_recv.at[w, s], x_rsem.at[w, s]).wait()
        both = x_recv[w, 0].astype(F32)
        for s in range(1, 4):
            both += x_recv[w, s].astype(F32)
        for zz in range(N_Z):
            block16 = both[:, zz * col : (zz + 1) * col].astype(BF16)
            z_send[w, zz] = jnp.concatenate([block16, gap], axis=1)

        def z_start(i, _):
            zz = lax.rem(z + far_first(i), N_Z)

            @pl.when(jnp.logical_not(is_here(w, zz)))
            def _():
                z_copy(w, zz).start()

            @pl.when(is_here(w, zz))
            def _():
                z_recv[xl, zz] = z_send[w, zz]
            return 0

        lax.fori_loop(0, N_Z, z_start, 0)

    collect_all(1)
    collect_all(2)
    left((4, 3))
    @pl.when(active)
    def _():
        for t in range(3):
            gone(done.at[t, : N_CP - 1], ret_send.at[t])

    gone(dv_buf.at[:, : 3 * SPAN], y_ssem.at[0])
    for w in range(2):
        half_copy(w).wait_send()
        for o in range(1, 4):
            across_copy(w, lax.rem(across[w] + o, 4)).wait_send()

    def all_blocks(buf, side, sem):
        pl.when(xl == side)(lambda: gone(buf.at[side, : N_Z - 1], sem.at[side]))
        pl.when(xl != side)(lambda: gone(buf.at[side], sem.at[side]))

    for xs in range(2):
        all_blocks(z_recv, xs, z_rsem)
        rs = slice(xs * piece, (xs + 1) * piece)
        total[rs] = sum(z_recv[xs, zz][:, :col].astype(F32) for zz in range(N_Z))
    last = pltpu.make_async_copy(total, dw_out, out_sem.at[3])
    last.start()

    for w in range(2):
        all_blocks(z_send, w, z_ssem)
    for t in range(3):
        pltpu.make_async_copy(back.at[t], outs[t].at[0], out_sem.at[t]).wait()
    last.wait()


def hand_over_kernel(*refs):
    ins, outs, bufs, sems = refs[:4], refs[4:8], refs[8:12], refs[12]
    first = [pltpu.make_async_copy(a, b, sems.at[0, i]) for i, (a, b) in enumerate(zip(ins, bufs))]
    then = [pltpu.make_async_copy(b, a, sems.at[1, i]) for i, (a, b) in enumerate(zip(outs, bufs))]
    for c in first:
        c.start()
    for c, d in zip(first, then):
        c.wait()
        d.start()
    for d in then:
        d.wait()


def hand_over(*arrays):
    any_spec = pl.BlockSpec(memory_space=pl.ANY)
    return pl.pallas_call(
        hand_over_kernel,
        out_shape=tuple(jax.ShapeDtypeStruct(a.shape, a.dtype) for a in arrays),
        in_specs=[any_spec] * 4,
        out_specs=(any_spec,) * 4,
        scratch_shapes=[pltpu.VMEM(a.shape, a.dtype) for a in arrays]
        + [pltpu.SemaphoreType.DMA((2, 4))],
        name="hand_over",
    )(*arrays)


def on_device(features, query_rows, key_rows, value_rows, attn_output, grad_output, log_sums):
    _, rows, width = query_rows.shape
    feat = features.shape[2]
    seq = N_CP * rows
    blk, half_w = feat // 16, width // 2
    any_spec = pl.BlockSpec(memory_space=pl.ANY)
    block = pltpu.VMEM((N_CP, rows, SPAN), BF16)
    out = jax.ShapeDtypeStruct(query_rows.shape, BF16)
    dma = pltpu.SemaphoreType.DMA
    results = pl.pallas_call(
        functools.partial(step_kernel, scale=SPAN**-0.5, rows=rows),
        out_shape=(out, out, out, jax.ShapeDtypeStruct((blk, half_w // N_Z), F32)),
        in_specs=[any_spec] * 7,
        out_specs=(any_spec,) * 4,
        scratch_shapes=[
            block, block, block, block,
            pltpu.VMEM((N_CP, 8, rows), F32),
            pltpu.VMEM((seq, seq), F32),
            pltpu.VMEM((seq, SPAN), F32),
            pltpu.VMEM((3, N_CP, rows, SPAN), BF16),
            pltpu.VMEM((3, rows, width), BF16),
            pltpu.VMEM((rows, width), BF16),
            pltpu.VMEM((rows, width), BF16),
            pltpu.VMEM((HEADS, 1, rows), F32),
            pltpu.VMEM((HEADS, 8, rows), F32),
            pltpu.VMEM((rows, feat), BF16),
            pltpu.VMEM((feat, rows), BF16),
            pltpu.VMEM((2, 4, feat // 4, rows), BF16),
            pltpu.VMEM((2, feat // 4, 4 * rows), BF16),
            pltpu.VMEM((2, 4 * rows, half_w), BF16),
            pltpu.VMEM((2, 2 * blk, half_w), BF16),
            pltpu.VMEM((2, 2 * blk, half_w), BF16),
            pltpu.VMEM((2 * blk, half_w), F32),
            pltpu.VMEM((2, 4, blk // 2, half_w), BF16),
            pltpu.VMEM((2, 4, blk // 2, half_w), BF16),
            pltpu.VMEM((2, N_Z, blk // 2, SPAN), BF16),
            pltpu.VMEM((2, N_Z, blk // 2, SPAN), BF16),
            pltpu.VMEM((blk, half_w // N_Z), F32),
            dma((4,)),
            dma((5,)), dma((5,)), dma((2, N_Z)), dma((3,)), dma((3,)), dma((HEADS,)), dma((4,)),
            dma((2, 4)), dma((2, 4)), dma((1,)), dma((2, 4)), dma((2,)), dma((2,)),
            dma((2, 4)), dma((2, 4)), dma((2,)), dma((2,)),
        ],
        compiler_params=pltpu.CompilerParams(
            collective_id=0, has_side_effects=True, vmem_limit_bytes=60 * 2**20),
        name="step",
    )(features, query_rows, key_rows, value_rows, attn_output, grad_output,
      jnp.transpose(log_sums, (2, 0, 1)))
    return hand_over(*results)


def solution(mesh):
    finer = Mesh(mesh.devices.reshape(2, 4, 2, 2, 8), AXES)
    rows = P(FSDP, CP, None)
    return jax.shard_map(
        on_device, mesh=finer, in_specs=(rows,) * 7,
        out_specs=(rows, rows, rows, P(FSDP, CP)), check_vma=False,
    )
```

```python
import functools

import jax
import jax.numpy as jnp
from jax import lax
from jax.experimental import pallas as pl
from jax.experimental.pallas import tpu as pltpu
from jax.sharding import Mesh
from jax.sharding import PartitionSpec as P

AXES = ("x_hi", "y", "core", "x_lo", "z")
FSDP = ("x_hi", "y", "core")
CP = ("x_lo", "z")
LOG2E = 1.4426950408889634
HEADS = 10
HALF = HEADS // 2
SPAN = 128
N_CP = 16
N_Z = 8
MESH = pl.DeviceIdType.MESH
F32 = jnp.float32
BF16 = jnp.bfloat16
NT = (((1,), (1,)), ((), ()))
TN = (((0,), (0,)), ((), ()))


def owner_of(head, parity):
    spare = head >= N_Z
    z = jnp.where(spare, 2 * parity + 4 * (head - N_Z), head)
    x = jnp.where(spare, 1 - parity, lax.rem(head + parity, 2))
    return x, z


def head_of(x, z, parity):
    first = x == lax.rem(z + parity, 2)
    spare = jnp.where(z == 2 * parity, N_Z, jnp.where(z == 2 * parity + 4, N_Z + 1, HEADS))
    return jnp.where(first, z, spare)


def step_kernel(
    f_in, q_in, k_in, v_in, o_in, g_in, l_in, dq_out, dk_out, dv_out, dw_out,
    q_buf, k_buf, v_buf, g_buf, s_buf, prob, dq_acc, done, back,
    g_own, o_own, l_own, s_own, f_own, ft_own, ft_out, ft_buf, dv_buf,
    half_send, half_recv, part, x_send, x_recv, z_send, z_recv, total,
    in_sem, send_sem, recv_sem, pair_sem, ret_send, ret_recv, value_sem, out_sem,
    f_ssem, f_rsem, y_ssem, y_rsem, d_ssem, d_rsem, x_ssem, x_rsem, z_ssem, z_rsem,
    *, scale, rows
):
    xh, y, core = lax.axis_index("x_hi"), lax.axis_index("y"), lax.axis_index("core")
    xl, z = lax.axis_index("x_lo"), lax.axis_index("z")
    x = 2 * xh + xl
    me = 2 * z + xl
    mine = head_of(xl, z, core)
    active = mine < HEADS
    feat = f_in.shape[2]
    half_w = q_in.shape[2] // 2
    blk = feat // 16
    piece = blk // 2
    col = half_w // N_Z

    def cp_id(peer):
        return {"x_lo": lax.rem(peer, 2), "z": peer // 2}

    def row_id(p):
        return {"x_hi": p // 2, "x_lo": lax.rem(p, 2)}

    def y_id(p):
        return {"y": p}

    near, near_id = (y, x), (y_id, row_id)
    across, across_id = (x, y), (row_id, y_id)

    loads = [
        pltpu.make_async_copy(g_in.at[0], g_own, in_sem.at[0]),
        pltpu.make_async_copy(o_in.at[0], o_own, in_sem.at[1]),
        pltpu.make_async_copy(l_in, l_own, in_sem.at[2]),
        pltpu.make_async_copy(f_in.at[0], f_own, in_sem.at[3]),
    ]
    for c in loads:
        c.start()

    barrier = pltpu.get_barrier_semaphore()

    def signal(where):
        pl.semaphore_signal(barrier, inc=1, device_id=where, device_id_type=MESH)

    def greet_cp(j, _):
        signal(cp_id(lax.rem(me + j, N_CP)))
        return 0

    def greet_quad(j, _):
        signal({"y": lax.rem(y + j, 4)})
        signal(row_id(lax.rem(x + j, 4)))
        return 0

    lax.fori_loop(1, N_CP, greet_cp, 0)
    lax.fori_loop(1, 4, greet_quad, 0)
    signal({"core": 1 - core})
    pl.semaphore_wait(barrier, N_CP + 6)

    def far_first(i):
        return jnp.where(lax.rem(i, 2) == 0, 4 + i // 2, 3 - i // 2) % N_Z

    def head_at(i):
        return jnp.where(i < 2, N_Z + i, lax.rem(z + far_first(i - 2), N_Z))

    def cols_of(head):
        return pl.ds(pl.multiple_of(head * SPAN, SPAN), SPAN)

    ins = (k_in, q_in, g_in, v_in)
    bufs = (k_buf, q_buf, g_buf, v_buf)

    def source(t, head):
        return ins[t].at[0, :, cols_of(head)] if t < 4 else s_own.at[head]

    def target(t, block):
        return bufs[t].at[block] if t < 4 else s_buf.at[block]

    def landed(t, b):
        return pair_sem.at[0 if t == 0 else 1, b] if t in (0, 3) else recv_sem.at[t]

    def send_all(kinds):
        def send(i, _):
            head = head_at(i)
            ox, oz = owner_of(head, core)

            @pl.when(head != mine)
            def _():
                for t in kinds:
                    pltpu.make_async_remote_copy(
                        src_ref=source(t, head), dst_ref=target(t, me),
                        send_sem=send_sem.at[t], recv_sem=landed(t, z),
                        device_id={"x_lo": ox, "z": oz}, device_id_type=MESH).start()

            @pl.when(head == mine)
            def _():
                for t in kinds:
                    if t < 4:
                        pltpu.make_async_copy(source(t, head), target(t, me), landed(t, z)).start()
                    else:
                        s_buf[me] = s_own[head]

            return 0

        lax.fori_loop(0, HEADS, send, 0)

    send_all((1, 2))

    for c in loads[:3]:
        c.wait()
    lse = l_own[...] * LOG2E
    s_own[...] = jnp.zeros_like(s_own)
    for h in range(HEADS):
        hs = slice(h * SPAN, (h + 1) * SPAN)
        product = g_own[:, hs].astype(F32) * o_own[:, hs].astype(F32)
        s_own[h, 0:1, :] = lse[h]
        s_own[h, 1:2, :] = jnp.sum(product.T, axis=0, keepdims=True)
    send_all((4,))
    send_all((0,))

    loads[3].wait()

    def turn(i, _):
        at = pl.multiple_of(i * SPAN, SPAN)
        ft_own[pl.ds(at, SPAN), :] = f_own[:, pl.ds(at, SPAN)].T
        return 0

    lax.fori_loop(0, feat // SPAN, turn, 0)

    def sort(i, _):
        f, part_s = i // 2, lax.rem(i, 2)
        of_y, of_x, of_core = lax.rem(f // 2, 4), 2 * (f // 8) + part_s, lax.rem(f, 2)
        value = ft_own[pl.ds(pl.multiple_of(i * piece, piece), piece), :]
        ft_out[0, of_y, pl.ds(pl.multiple_of((of_core * 4 + of_x) * piece, piece), piece), :] = value
        ft_out[1, of_x, pl.ds(pl.multiple_of((of_core * 4 + of_y) * piece, piece), piece), :] = value
        return 0

    lax.fori_loop(0, feat // piece, sort, 0)

    def my_span(w):
        return pl.ds(pl.multiple_of(near[w] * SPAN, SPAN), SPAN)

    def feature_copy(w, j):
        to = lax.rem(near[w] + j, 4)
        return pltpu.make_async_remote_copy(
            src_ref=ft_out.at[w, to], dst_ref=ft_buf.at[w, :, my_span(w)],
            send_sem=f_ssem.at[w, j], recv_sem=f_rsem.at[w, j], device_id=near_id[w](to),
            device_id_type=MESH)

    for w in range(2):
        for j in range(1, 4):
            feature_copy(w, j).start()
        ft_buf[w, :, my_span(w)] = ft_out[w, near[w]]

    def gone(ref, sem):
        pltpu.make_async_copy(ref, ref, sem).wait()

    def left(kinds):
        def count(n):
            for t in kinds:
                gone(ins[t].at[0, :, : n * SPAN] if t < 4 else s_own.at[:n], send_sem.at[t])

        pl.when(active)(lambda: count(HEADS - 1))
        pl.when(jnp.logical_not(active))(lambda: count(HEADS))

    left((1, 2))
    left((0,))

    def value_copy(w, h, o):
        return pltpu.make_async_remote_copy(
            src_ref=back.at[0, :, cols_of(h)],
            dst_ref=dv_buf.at[w, my_span(w), cols_of(h - HALF * w)],
            send_sem=y_ssem.at[0], recv_sem=y_rsem.at[w, near[w]],
            device_id=near_id[w](lax.rem(near[w] + o, 4)), device_id_type=MESH)

    def pass_on(i, _):
        h = jnp.where(i < N_Z, lax.rem(z + far_first(i), N_Z), i)

        @pl.when(h != mine)
        def _():
            gone(back.at[0, :, cols_of(h)], value_sem.at[h])

        for w in range(2):
            @pl.when(h // HALF == w)
            def _():
                for o in range(1, 4):
                    value_copy(w, h, o).start()
        return 0

    UB = 2
    seq = N_CP * rows

    def block_at(i):
        return lax.rem(z + N_Z - far_first(i), N_Z)

    def arrive_pair(t, b):
        gone(bufs[t].at[pl.ds(2 * b, 2)], landed(t, b))

    def give(t, r):
        @pl.when(r != me)
        def _():
            pltpu.make_async_remote_copy(
                src_ref=done.at[t, r], dst_ref=back.at[t, :, cols_of(mine)],
                send_sem=ret_send.at[t], recv_sem=value_sem.at[mine] if t == 0 else ret_recv.at[t],
                device_id=cp_id(r), device_id_type=MESH).start()

        @pl.when(r == me)
        def _():
            back[t, :, cols_of(mine)] = done[t, me]

    @pl.when(active)
    def _():
        gone(q_buf, recv_sem.at[1])
        gone(g_buf, recv_sem.at[2])
        gone(s_buf.at[: N_CP - 1], recv_sem.at[4])
        lse = jnp.concatenate([s_buf[i, 0:1, :] for i in range(N_CP)], axis=1)

        def value_step(i, _):
            b = block_at(i)
            us = pl.ds(b * UB, UB)
            arrive_pair(0, b)
            k = k_buf[us].reshape(UB * rows, SPAN)
            st = lax.dot_general(k, q_buf[...].reshape(seq, SPAN), NT, preferred_element_type=F32)
            p = jnp.exp2(st * (scale * LOG2E) - lse)
            prob[pl.ds(pl.multiple_of(b * UB * rows, UB * rows), UB * rows), :] = p
            dv = jnp.dot(p.astype(BF16), g_buf[...].reshape(seq, SPAN), preferred_element_type=F32)
            done[0, us] = dv.astype(BF16).reshape(UB, rows, SPAN)
            give(0, 2 * b)
            give(0, 2 * b + 1)
            return 0

        lax.fori_loop(0, N_CP // UB, value_step, 0)
        dq_acc[...] = jnp.zeros_like(dq_acc)


    def key_step(i):
        b = block_at(i)
        us = pl.ds(b * UB, UB)
        arrive_pair(3, b)
        k = k_buf[us].reshape(UB * rows, SPAN)
        v = v_buf[us].reshape(UB * rows, SPAN)
        delta = jnp.concatenate([s_buf[i, 1:2, :] for i in range(N_CP)], axis=1)
        p = prob[pl.ds(pl.multiple_of(b * UB * rows, UB * rows), UB * rows), :]
        dp = lax.dot_general(v, g_buf[...].reshape(seq, SPAN), NT, preferred_element_type=F32)
        ds = (p * (dp - delta)).astype(BF16)
        dk = jnp.dot(ds, q_buf[...].reshape(seq, SPAN), preferred_element_type=F32)
        done[1, us] = (dk * scale).astype(BF16).reshape(UB, rows, SPAN)
        dq_acc[...] += lax.dot_general(ds, k, TN, preferred_element_type=F32)
        give(1, 2 * b)
        give(1, 2 * b + 1)

    def key_steps(lo, hi):
        def one(i, _):
            @pl.when(active)
            def _():
                key_step(i)
            return 0

        lax.fori_loop(lo, hi, one, 0)

    def finish_queries():
        done[2] = (dq_acc[...] * scale).astype(BF16).reshape(N_CP, rows, SPAN)

        def query_give(i, _):
            b = block_at(i)
            give(2, 2 * b)
            give(2, 2 * b + 1)
            return 0

        lax.fori_loop(0, N_Z, query_give, 0)

    def passes(lo, hi):
        lax.fori_loop(lo, hi, pass_on, 0)

    passes(0, 1)
    send_all((3,))
    passes(1, HEADS)
    key_steps(0, N_Z)
    pl.when(active)(finish_queries)

    outs = (dv_out, dk_out, dq_out)

    def collect_all(t):
        pl.when(active)(lambda: gone(back.at[t, :, : (HEADS - 1) * SPAN], ret_recv.at[t]))
        pl.when(jnp.logical_not(active))(lambda: gone(back.at[t], ret_recv.at[t]))
        pltpu.make_async_copy(back.at[t], outs[t].at[0], out_sem.at[t]).start()

    pltpu.make_async_copy(back.at[0], outs[0].at[0], out_sem.at[0]).start()

    for w in range(2):
        dv_buf[w, my_span(w), :] = back[0, :, w * half_w : (w + 1) * half_w]
    for w in range(2):
        for j in range(1, 4):
            feature_copy(w, j).wait()

    def values_from(w):
        for o in range(1, 4):
            peer = lax.rem(near[w] + o, 4)
            gone(dv_buf.at[w, pl.ds(pl.multiple_of(peer * SPAN, SPAN), SPAN), :], y_rsem.at[w, peer])

    def part_of(w, which):
        rs = pl.ds(pl.multiple_of(which * 2 * blk, 2 * blk), 2 * blk)
        return jnp.dot(ft_buf[w, rs, :], dv_buf[w], preferred_element_type=F32)

    def half_copy(w):
        return pltpu.make_async_remote_copy(
            src_ref=half_send.at[w], dst_ref=half_recv.at[w], send_sem=d_ssem.at[w],
            recv_sem=d_rsem.at[w], device_id={"core": 1 - core}, device_id_type=MESH)

    def across_copy(w, j):
        return pltpu.make_async_remote_copy(
            src_ref=x_send.at[w, j], dst_ref=x_recv.at[w, across[w]], send_sem=x_ssem.at[w, j],
            recv_sem=x_rsem.at[w, across[w]], device_id=across_id[w](j), device_id_type=MESH)

    for w in range(2):
        values_from(w)
        half_send[w] = part_of(w, 1 - core).astype(BF16)
        half_copy(w).start()
        part[...] = part_of(w, core)
        half_copy(w).wait_recv()
        both = (part[...] + half_recv[w].astype(F32)).astype(BF16)
        x_send[w] = both.reshape(4, piece, half_w)
        for o in range(1, 4):
            across_copy(w, lax.rem(across[w] + o, 4)).start()
        x_recv[w, across[w]] = x_send[w, across[w]]

    def z_copy(w, zz):
        return pltpu.make_async_remote_copy(
            src_ref=z_send.at[w, zz], dst_ref=z_recv.at[xl, z], send_sem=z_ssem.at[w],
            recv_sem=z_rsem.at[xl], device_id={"x_lo": w, "z": zz}, device_id_type=MESH)

    def is_here(w, zz):
        return jnp.logical_and(xl == w, zz == z)

    gap = jnp.zeros((piece, SPAN - col), BF16)
    for w in range(2):
        for o in range(1, 4):
            s = lax.rem(across[w] + o, 4)
            pltpu.make_async_copy(x_send.at[w, s], x_recv.at[w, s], x_rsem.at[w, s]).wait()
        both = x_recv[w, 0].astype(F32)
        for s in range(1, 4):
            both += x_recv[w, s].astype(F32)
        for zz in range(N_Z):
            block16 = both[:, zz * col : (zz + 1) * col].astype(BF16)
            z_send[w, zz] = jnp.concatenate([block16, gap], axis=1)

        def z_start(i, _):
            zz = lax.rem(z + far_first(i), N_Z)

            @pl.when(jnp.logical_not(is_here(w, zz)))
            def _():
                z_copy(w, zz).start()

            @pl.when(is_here(w, zz))
            def _():
                z_recv[xl, zz] = z_send[w, zz]
            return 0

        lax.fori_loop(0, N_Z, z_start, 0)

    collect_all(1)
    collect_all(2)
    left((4, 3))
    @pl.when(active)
    def _():
        for t in range(3):
            gone(done.at[t, : N_CP - 1], ret_send.at[t])

    gone(dv_buf.at[:, : 3 * SPAN], y_ssem.at[0])
    for w in range(2):
        half_copy(w).wait_send()
        for o in range(1, 4):
            across_copy(w, lax.rem(across[w] + o, 4)).wait_send()

    def all_blocks(buf, side, sem):
        pl.when(xl == side)(lambda: gone(buf.at[side, : N_Z - 1], sem.at[side]))
        pl.when(xl != side)(lambda: gone(buf.at[side], sem.at[side]))

    for xs in range(2):
        all_blocks(z_recv, xs, z_rsem)
        rs = slice(xs * piece, (xs + 1) * piece)
        total[rs] = sum(z_recv[xs, zz][:, :col].astype(F32) for zz in range(N_Z))
    last = pltpu.make_async_copy(total, dw_out, out_sem.at[3])
    last.start()

    for w in range(2):
        all_blocks(z_send, w, z_ssem)
    for t in range(3):
        pltpu.make_async_copy(back.at[t], outs[t].at[0], out_sem.at[t]).wait()
    last.wait()


def hand_over_kernel(*refs):
    ins, outs, bufs, sems = refs[:4], refs[4:8], refs[8:12], refs[12]
    first = [pltpu.make_async_copy(a, b, sems.at[0, i]) for i, (a, b) in enumerate(zip(ins, bufs))]
    then = [pltpu.make_async_copy(b, a, sems.at[1, i]) for i, (a, b) in enumerate(zip(outs, bufs))]
    for c in first:
        c.start()
    for c, d in zip(first, then):
        c.wait()
        d.start()
    for d in then:
        d.wait()


def hand_over(*arrays):
    any_spec = pl.BlockSpec(memory_space=pl.ANY)
    return pl.pallas_call(
        hand_over_kernel,
        out_shape=tuple(jax.ShapeDtypeStruct(a.shape, a.dtype) for a in arrays),
        in_specs=[any_spec] * 4,
        out_specs=(any_spec,) * 4,
        scratch_shapes=[pltpu.VMEM(a.shape, a.dtype) for a in arrays]
        + [pltpu.SemaphoreType.DMA((2, 4))],
        name="hand_over",
    )(*arrays)


def on_device(features, query_rows, key_rows, value_rows, attn_output, grad_output, log_sums):
    _, rows, width = query_rows.shape
    feat = features.shape[2]
    seq = N_CP * rows
    blk, half_w = feat // 16, width // 2
    any_spec = pl.BlockSpec(memory_space=pl.ANY)
    block = pltpu.VMEM((N_CP, rows, SPAN), BF16)
    out = jax.ShapeDtypeStruct(query_rows.shape, BF16)
    dma = pltpu.SemaphoreType.DMA
    results = pl.pallas_call(
        functools.partial(step_kernel, scale=SPAN**-0.5, rows=rows),
        out_shape=(out, out, out, jax.ShapeDtypeStruct((blk, half_w // N_Z), F32)),
        in_specs=[any_spec] * 7,
        out_specs=(any_spec,) * 4,
        scratch_shapes=[
            block, block, block, block,
            pltpu.VMEM((N_CP, 8, rows), F32),
            pltpu.VMEM((seq, seq), F32),
            pltpu.VMEM((seq, SPAN), F32),
            pltpu.VMEM((3, N_CP, rows, SPAN), BF16),
            pltpu.VMEM((3, rows, width), BF16),
            pltpu.VMEM((rows, width), BF16),
            pltpu.VMEM((rows, width), BF16),
            pltpu.VMEM((HEADS, 1, rows), F32),
            pltpu.VMEM((HEADS, 8, rows), F32),
            pltpu.VMEM((rows, feat), BF16),
            pltpu.VMEM((feat, rows), BF16),
            pltpu.VMEM((2, 4, feat // 4, rows), BF16),
            pltpu.VMEM((2, feat // 4, 4 * rows), BF16),
            pltpu.VMEM((2, 4 * rows, half_w), BF16),
            pltpu.VMEM((2, 2 * blk, half_w), BF16),
            pltpu.VMEM((2, 2 * blk, half_w), BF16),
            pltpu.VMEM((2 * blk, half_w), F32),
            pltpu.VMEM((2, 4, blk // 2, half_w), BF16),
            pltpu.VMEM((2, 4, blk // 2, half_w), BF16),
            pltpu.VMEM((2, N_Z, blk // 2, SPAN), BF16),
            pltpu.VMEM((2, N_Z, blk // 2, SPAN), BF16),
            pltpu.VMEM((blk, half_w // N_Z), F32),
            dma((4,)),
            dma((5,)), dma((5,)), dma((2, N_Z)), dma((3,)), dma((3,)), dma((HEADS,)), dma((4,)),
            dma((2, 4)), dma((2, 4)), dma((1,)), dma((2, 4)), dma((2,)), dma((2,)),
            dma((2, 4)), dma((2, 4)), dma((2,)), dma((2,)),
        ],
        compiler_params=pltpu.CompilerParams(
            collective_id=0, has_side_effects=True, vmem_limit_bytes=60 * 2**20),
        name="step",
    )(features, query_rows, key_rows, value_rows, attn_output, grad_output,
      jnp.transpose(log_sums, (2, 0, 1)))
    return hand_over(*results)


def solution(mesh):
    finer = Mesh(mesh.devices.reshape(2, 4, 2, 2, 8), AXES)
    rows = P(FSDP, CP, None)
    return jax.shard_map(
        on_device, mesh=finer, in_specs=(rows,) * 7,
        out_specs=(rows, rows, rows, P(FSDP, CP)), check_vma=False,
    )
```

```python
import functools

import jax
import jax.numpy as jnp
from jax import lax
from jax.experimental import pallas as pl
from jax.experimental.pallas import tpu as pltpu
from jax.sharding import Mesh
from jax.sharding import PartitionSpec as P

AXES = ("x_hi", "y", "core", "x_lo", "z")
FSDP = ("x_hi", "y", "core")
CP = ("x_lo", "z")
LOG2E = 1.4426950408889634
HEADS = 10
HALF = HEADS // 2
SPAN = 128
N_CP = 16
N_Z = 8
MESH = pl.DeviceIdType.MESH
F32 = jnp.float32
BF16 = jnp.bfloat16
NT = (((1,), (1,)), ((), ()))
TN = (((0,), (0,)), ((), ()))


def owner_of(head, parity):
    spare = head >= N_Z
    z = jnp.where(spare, 2 * parity + 4 * (head - N_Z), head)
    x = jnp.where(spare, 1 - parity, lax.rem(head + parity, 2))
    return x, z


def head_of(x, z, parity):
    first = x == lax.rem(z + parity, 2)
    spare = jnp.where(z == 2 * parity, N_Z, jnp.where(z == 2 * parity + 4, N_Z + 1, HEADS))
    return jnp.where(first, z, spare)


def step_kernel(
    f_in, q_in, k_in, v_in, o_in, g_in, l_in, dq_out, dk_out, dv_out, dw_out,
    q_buf, k_buf, v_buf, g_buf, s_buf, prob, dq_acc, done, back,
    g_own, o_own, l_own, s_own, f_own, ft_own, ft_out, ft_buf, dv_buf,
    half_send, half_recv, part, x_send, x_recv, z_send, z_recv, total,
    in_sem, send_sem, recv_sem, pair_sem, ret_send, ret_recv, value_sem, out_sem,
    f_ssem, f_rsem, y_ssem, y_rsem, d_ssem, d_rsem, x_ssem, x_rsem, z_ssem, z_rsem,
    *, scale, rows
):
    xh, y, core = lax.axis_index("x_hi"), lax.axis_index("y"), lax.axis_index("core")
    xl, z = lax.axis_index("x_lo"), lax.axis_index("z")
    x = 2 * xh + xl
    me = 2 * z + xl
    mine = head_of(xl, z, core)
    active = mine < HEADS
    feat = f_in.shape[2]
    half_w = q_in.shape[2] // 2
    blk = feat // 16
    piece = blk // 2
    col = half_w // N_Z

    def cp_id(peer):
        return {"x_lo": lax.rem(peer, 2), "z": peer // 2}

    def row_id(p):
        return {"x_hi": p // 2, "x_lo": lax.rem(p, 2)}

    def y_id(p):
        return {"y": p}

    near, near_id = (y, x), (y_id, row_id)
    across, across_id = (x, y), (row_id, y_id)

    loads = [
        pltpu.make_async_copy(g_in.at[0], g_own, in_sem.at[0]),
        pltpu.make_async_copy(o_in.at[0], o_own, in_sem.at[1]),
        pltpu.make_async_copy(l_in, l_own, in_sem.at[2]),
        pltpu.make_async_copy(f_in.at[0], f_own, in_sem.at[3]),
    ]
    for c in loads:
        c.start()

    barrier = pltpu.get_barrier_semaphore()

    def signal(where):
        pl.semaphore_signal(barrier, inc=1, device_id=where, device_id_type=MESH)

    def greet_cp(j, _):
        signal(cp_id(lax.rem(me + j, N_CP)))
        return 0

    def greet_quad(j, _):
        signal({"y": lax.rem(y + j, 4)})
        signal(row_id(lax.rem(x + j, 4)))
        return 0

    lax.fori_loop(1, N_CP, greet_cp, 0)
    lax.fori_loop(1, 4, greet_quad, 0)
    signal({"core": 1 - core})
    pl.semaphore_wait(barrier, N_CP + 6)

    def far_first(i):
        return jnp.where(lax.rem(i, 2) == 0, 4 + i // 2, 3 - i // 2) % N_Z

    def head_at(i):
        return jnp.where(i < 2, N_Z + i, lax.rem(z + far_first(i - 2), N_Z))

    def cols_of(head):
        return pl.ds(pl.multiple_of(head * SPAN, SPAN), SPAN)

    ins = (k_in, q_in, g_in, v_in)
    bufs = (k_buf, q_buf, g_buf, v_buf)

    def source(t, head):
        return ins[t].at[0, :, cols_of(head)] if t < 4 else s_own.at[head]

    def target(t, block):
        return bufs[t].at[block] if t < 4 else s_buf.at[block]

    def landed(t, b):
        return pair_sem.at[0 if t == 0 else 1, b] if t in (0, 3) else recv_sem.at[t]

    def send_all(kinds):
        def send(i, _):
            head = head_at(i)
            ox, oz = owner_of(head, core)

            @pl.when(head != mine)
            def _():
                for t in kinds:
                    pltpu.make_async_remote_copy(
                        src_ref=source(t, head), dst_ref=target(t, me),
                        send_sem=send_sem.at[t], recv_sem=landed(t, z),
                        device_id={"x_lo": ox, "z": oz}, device_id_type=MESH).start()

            @pl.when(head == mine)
            def _():
                for t in kinds:
                    if t < 4:
                        pltpu.make_async_copy(source(t, head), target(t, me), landed(t, z)).start()
                    else:
                        s_buf[me] = s_own[head]

            return 0

        lax.fori_loop(0, HEADS, send, 0)

    send_all((1, 2))

    for c in loads[:3]:
        c.wait()
    lse = l_own[...] * LOG2E
    s_own[...] = jnp.zeros_like(s_own)
    for h in range(HEADS):
        hs = slice(h * SPAN, (h + 1) * SPAN)
        product = g_own[:, hs].astype(F32) * o_own[:, hs].astype(F32)
        s_own[h, 0:1, :] = lse[h]
        s_own[h, 1:2, :] = jnp.sum(product.T, axis=0, keepdims=True)
    send_all((4,))
    send_all((0,))

    loads[3].wait()

    def turn(i, _):
        at = pl.multiple_of(i * SPAN, SPAN)
        ft_own[pl.ds(at, SPAN), :] = f_own[:, pl.ds(at, SPAN)].T
        return 0

    lax.fori_loop(0, feat // SPAN, turn, 0)

    def sort(i, _):
        f, part_s = i // 2, lax.rem(i, 2)
        of_y, of_x, of_core = lax.rem(f // 2, 4), 2 * (f // 8) + part_s, lax.rem(f, 2)
        value = ft_own[pl.ds(pl.multiple_of(i * piece, piece), piece), :]
        ft_out[0, of_y, pl.ds(pl.multiple_of((of_core * 4 + of_x) * piece, piece), piece), :] = value
        ft_out[1, of_x, pl.ds(pl.multiple_of((of_core * 4 + of_y) * piece, piece), piece), :] = value
        return 0

    lax.fori_loop(0, feat // piece, sort, 0)

    def my_span(w):
        return pl.ds(pl.multiple_of(near[w] * SPAN, SPAN), SPAN)

    def feature_copy(w, j):
        to = lax.rem(near[w] + j, 4)
        return pltpu.make_async_remote_copy(
            src_ref=ft_out.at[w, to], dst_ref=ft_buf.at[w, :, my_span(w)],
            send_sem=f_ssem.at[w, j], recv_sem=f_rsem.at[w, j], device_id=near_id[w](to),
            device_id_type=MESH)

    for w in range(2):
        if w == 0:
            for j in range(1, 4):
                feature_copy(w, j).start()
        ft_buf[w, :, my_span(w)] = ft_out[w, near[w]]

    def gone(ref, sem):
        pltpu.make_async_copy(ref, ref, sem).wait()

    def left(kinds):
        def count(n):
            for t in kinds:
                gone(ins[t].at[0, :, : n * SPAN] if t < 4 else s_own.at[:n], send_sem.at[t])

        pl.when(active)(lambda: count(HEADS - 1))
        pl.when(jnp.logical_not(active))(lambda: count(HEADS))

    left((1, 2))
    for j in range(1, 4):
        feature_copy(1, j).start()
    left((0,))

    def value_copy(w, h, o):
        return pltpu.make_async_remote_copy(
            src_ref=back.at[0, :, cols_of(h)],
            dst_ref=dv_buf.at[w, my_span(w), cols_of(h - HALF * w)],
            send_sem=y_ssem.at[0], recv_sem=y_rsem.at[w, near[w]],
            device_id=near_id[w](lax.rem(near[w] + o, 4)), device_id_type=MESH)

    def pass_on(i, _):
        h = jnp.where(i < N_Z, lax.rem(z + far_first(i), N_Z), i)

        @pl.when(h != mine)
        def _():
            gone(back.at[0, :, cols_of(h)], value_sem.at[h])

        for w in range(2):
            @pl.when(h // HALF == w)
            def _():
                for o in range(1, 4):
                    value_copy(w, h, o).start()
        return 0

    UB = 2
    seq = N_CP * rows

    def block_at(i):
        return lax.rem(z + N_Z - far_first(i), N_Z)

    def arrive_pair(t, b):
        gone(bufs[t].at[pl.ds(2 * b, 2)], landed(t, b))

    def give(t, r):
        @pl.when(r != me)
        def _():
            pltpu.make_async_remote_copy(
                src_ref=done.at[t, r], dst_ref=back.at[t, :, cols_of(mine)],
                send_sem=ret_send.at[t], recv_sem=value_sem.at[mine] if t == 0 else ret_recv.at[t],
                device_id=cp_id(r), device_id_type=MESH).start()

        @pl.when(r == me)
        def _():
            back[t, :, cols_of(mine)] = done[t, me]

    @pl.when(active)
    def _():
        gone(q_buf, recv_sem.at[1])
        gone(g_buf, recv_sem.at[2])
        gone(s_buf.at[: N_CP - 1], recv_sem.at[4])
        lse = jnp.concatenate([s_buf[i, 0:1, :] for i in range(N_CP)], axis=1)

        def value_step(i, _):
            b = block_at(i)
            us = pl.ds(b * UB, UB)
            arrive_pair(0, b)
            k = k_buf[us].reshape(UB * rows, SPAN)
            st = lax.dot_general(k, q_buf[...].reshape(seq, SPAN), NT, preferred_element_type=F32)
            p = jnp.exp2(st * (scale * LOG2E) - lse)
            prob[pl.ds(pl.multiple_of(b * UB * rows, UB * rows), UB * rows), :] = p
            dv = jnp.dot(p.astype(BF16), g_buf[...].reshape(seq, SPAN), preferred_element_type=F32)
            done[0, us] = dv.astype(BF16).reshape(UB, rows, SPAN)
            give(0, 2 * b)
            give(0, 2 * b + 1)
            return 0

        lax.fori_loop(0, N_CP // UB, value_step, 0)
        dq_acc[...] = jnp.zeros_like(dq_acc)


    def key_step(i):
        b = block_at(i)
        us = pl.ds(b * UB, UB)
        arrive_pair(3, b)
        k = k_buf[us].reshape(UB * rows, SPAN)
        v = v_buf[us].reshape(UB * rows, SPAN)
        delta = jnp.concatenate([s_buf[i, 1:2, :] for i in range(N_CP)], axis=1)
        p = prob[pl.ds(pl.multiple_of(b * UB * rows, UB * rows), UB * rows), :]
        dp = lax.dot_general(v, g_buf[...].reshape(seq, SPAN), NT, preferred_element_type=F32)
        ds = (p * (dp - delta)).astype(BF16)
        dk = jnp.dot(ds, q_buf[...].reshape(seq, SPAN), preferred_element_type=F32)
        done[1, us] = (dk * scale).astype(BF16).reshape(UB, rows, SPAN)
        dq_acc[...] += lax.dot_general(k, ds, TN, preferred_element_type=F32)
        give(1, 2 * b)
        give(1, 2 * b + 1)

    def key_steps(lo, hi):
        def one(i, _):
            @pl.when(active)
            def _():
                key_step(i)
            return 0

        lax.fori_loop(lo, hi, one, 0)

    def finish_queries():
        done[2] = (dq_acc[...].T * scale).astype(BF16).reshape(N_CP, rows, SPAN)

        def query_give(i, _):
            b = block_at(i)
            give(2, 2 * b)
            give(2, 2 * b + 1)
            return 0

        lax.fori_loop(0, N_Z, query_give, 0)

    def passes(lo, hi):
        lax.fori_loop(lo, hi, pass_on, 0)

    send_all((3,))
    passes(0, HEADS)
    key_steps(0, N_Z)
    pl.when(active)(finish_queries)

    outs = (dv_out, dk_out, dq_out)

    def collect_all(t):
        pl.when(active)(lambda: gone(back.at[t, :, : (HEADS - 1) * SPAN], ret_recv.at[t]))
        pl.when(jnp.logical_not(active))(lambda: gone(back.at[t], ret_recv.at[t]))
        pltpu.make_async_copy(back.at[t], outs[t].at[0], out_sem.at[t]).start()

    pltpu.make_async_copy(back.at[0], outs[0].at[0], out_sem.at[0]).start()

    for w in range(2):
        dv_buf[w, my_span(w), :] = back[0, :, w * half_w : (w + 1) * half_w]
    for w in range(2):
        for j in range(1, 4):
            feature_copy(w, j).wait()

    def values_from(w):
        for o in range(1, 4):
            peer = lax.rem(near[w] + o, 4)
            gone(dv_buf.at[w, pl.ds(pl.multiple_of(peer * SPAN, SPAN), SPAN), :], y_rsem.at[w, peer])

    def part_of(w, which):
        rs = pl.ds(pl.multiple_of(which * 2 * blk, 2 * blk), 2 * blk)
        return jnp.dot(ft_buf[w, rs, :], dv_buf[w], preferred_element_type=F32)

    def half_copy(w):
        return pltpu.make_async_remote_copy(
            src_ref=half_send.at[w], dst_ref=half_recv.at[w], send_sem=d_ssem.at[w],
            recv_sem=d_rsem.at[w], device_id={"core": 1 - core}, device_id_type=MESH)

    def across_copy(w, j):
        return pltpu.make_async_remote_copy(
            src_ref=x_send.at[w, j], dst_ref=x_recv.at[w, across[w]], send_sem=x_ssem.at[w, j],
            recv_sem=x_rsem.at[w, across[w]], device_id=across_id[w](j), device_id_type=MESH)

    for w in range(2):
        values_from(w)
        half_send[w] = part_of(w, 1 - core).astype(BF16)
        half_copy(w).start()
        part[...] = part_of(w, core)
        half_copy(w).wait_recv()
        both = (part[...] + half_recv[w].astype(F32)).astype(BF16)
        x_send[w] = both.reshape(4, piece, half_w)
        for o in range(1, 4):
            across_copy(w, lax.rem(across[w] + o, 4)).start()
        x_recv[w, across[w]] = x_send[w, across[w]]

    def z_copy(w, zz):
        return pltpu.make_async_remote_copy(
            src_ref=z_send.at[w, zz], dst_ref=z_recv.at[xl, z], send_sem=z_ssem.at[w],
            recv_sem=z_rsem.at[xl], device_id={"x_lo": w, "z": zz}, device_id_type=MESH)

    def is_here(w, zz):
        return jnp.logical_and(xl == w, zz == z)

    gap = jnp.zeros((piece, SPAN - col), BF16)
    for w in range(2):
        for o in range(1, 4):
            s = lax.rem(across[w] + o, 4)
            pltpu.make_async_copy(x_send.at[w, s], x_recv.at[w, s], x_rsem.at[w, s]).wait()
        both = x_recv[w, 0].astype(F32)
        for s in range(1, 4):
            both += x_recv[w, s].astype(F32)
        for zz in range(N_Z):
            block16 = both[:, zz * col : (zz + 1) * col].astype(BF16)
            z_send[w, zz] = jnp.concatenate([block16, gap], axis=1)

        def z_start(i, _):
            zz = lax.rem(z + far_first(i), N_Z)

            @pl.when(jnp.logical_not(is_here(w, zz)))
            def _():
                z_copy(w, zz).start()

            @pl.when(is_here(w, zz))
            def _():
                z_recv[xl, zz] = z_send[w, zz]
            return 0

        lax.fori_loop(0, N_Z, z_start, 0)

    collect_all(1)
    collect_all(2)
    left((4, 3))
    @pl.when(active)
    def _():
        for t in range(3):
            gone(done.at[t, : N_CP - 1], ret_send.at[t])

    gone(dv_buf.at[:, : 3 * SPAN], y_ssem.at[0])
    for w in range(2):
        half_copy(w).wait_send()
        for o in range(1, 4):
            across_copy(w, lax.rem(across[w] + o, 4)).wait_send()

    def all_blocks(buf, side, sem):
        pl.when(xl == side)(lambda: gone(buf.at[side, : N_Z - 1], sem.at[side]))
        pl.when(xl != side)(lambda: gone(buf.at[side], sem.at[side]))

    for xs in range(2):
        all_blocks(z_recv, xs, z_rsem)
        rs = slice(xs * piece, (xs + 1) * piece)
        total[rs] = sum(z_recv[xs, zz][:, :col].astype(F32) for zz in range(N_Z))
    last = pltpu.make_async_copy(total, dw_out, out_sem.at[3])
    last.start()

    for w in range(2):
        all_blocks(z_send, w, z_ssem)
    for t in range(3):
        pltpu.make_async_copy(back.at[t], outs[t].at[0], out_sem.at[t]).wait()
    last.wait()


def hand_over_kernel(*refs):
    ins, outs, bufs, sems = refs[:4], refs[4:8], refs[8:12], refs[12]
    first = [pltpu.make_async_copy(a, b, sems.at[0, i]) for i, (a, b) in enumerate(zip(ins, bufs))]
    then = [pltpu.make_async_copy(b, a, sems.at[1, i]) for i, (a, b) in enumerate(zip(outs, bufs))]
    for c in first:
        c.start()
    for c, d in zip(first, then):
        c.wait()
        d.start()
    for d in then:
        d.wait()


def hand_over(*arrays):
    any_spec = pl.BlockSpec(memory_space=pl.ANY)
    return pl.pallas_call(
        hand_over_kernel,
        out_shape=tuple(jax.ShapeDtypeStruct(a.shape, a.dtype) for a in arrays),
        in_specs=[any_spec] * 4,
        out_specs=(any_spec,) * 4,
        scratch_shapes=[pltpu.VMEM(a.shape, a.dtype) for a in arrays]
        + [pltpu.SemaphoreType.DMA((2, 4))],
        name="hand_over",
    )(*arrays)


def on_device(features, query_rows, key_rows, value_rows, attn_output, grad_output, log_sums):
    _, rows, width = query_rows.shape
    feat = features.shape[2]
    seq = N_CP * rows
    blk, half_w = feat // 16, width // 2
    any_spec = pl.BlockSpec(memory_space=pl.ANY)
    block = pltpu.VMEM((N_CP, rows, SPAN), BF16)
    out = jax.ShapeDtypeStruct(query_rows.shape, BF16)
    dma = pltpu.SemaphoreType.DMA
    results = pl.pallas_call(
        functools.partial(step_kernel, scale=SPAN**-0.5, rows=rows),
        out_shape=(out, out, out, jax.ShapeDtypeStruct((blk, half_w // N_Z), F32)),
        in_specs=[any_spec] * 7,
        out_specs=(any_spec,) * 4,
        scratch_shapes=[
            block, block, block, block,
            pltpu.VMEM((N_CP, 8, rows), F32),
            pltpu.VMEM((seq, seq), F32),
            pltpu.VMEM((SPAN, seq), F32),
            pltpu.VMEM((3, N_CP, rows, SPAN), BF16),
            pltpu.VMEM((3, rows, width), BF16),
            pltpu.VMEM((rows, width), BF16),
            pltpu.VMEM((rows, width), BF16),
            pltpu.VMEM((HEADS, 1, rows), F32),
            pltpu.VMEM((HEADS, 8, rows), F32),
            pltpu.VMEM((rows, feat), BF16),
            pltpu.VMEM((feat, rows), BF16),
            pltpu.VMEM((2, 4, feat // 4, rows), BF16),
            pltpu.VMEM((2, feat // 4, 4 * rows), BF16),
            pltpu.VMEM((2, 4 * rows, half_w), BF16),
            pltpu.VMEM((2, 2 * blk, half_w), BF16),
            pltpu.VMEM((2, 2 * blk, half_w), BF16),
            pltpu.VMEM((2 * blk, half_w), F32),
            pltpu.VMEM((2, 4, blk // 2, half_w), BF16),
            pltpu.VMEM((2, 4, blk // 2, half_w), BF16),
            pltpu.VMEM((2, N_Z, blk // 2, SPAN), BF16),
            pltpu.VMEM((2, N_Z, blk // 2, SPAN), BF16),
            pltpu.VMEM((blk, half_w // N_Z), F32),
            dma((4,)),
            dma((5,)), dma((5,)), dma((2, N_Z)), dma((3,)), dma((3,)), dma((HEADS,)), dma((4,)),
            dma((2, 4)), dma((2, 4)), dma((1,)), dma((2, 4)), dma((2,)), dma((2,)),
            dma((2, 4)), dma((2, 4)), dma((2,)), dma((2,)),
        ],
        compiler_params=pltpu.CompilerParams(
            collective_id=0, has_side_effects=True, vmem_limit_bytes=60 * 2**20),
        name="step",
    )(features, query_rows, key_rows, value_rows, attn_output, grad_output,
      jnp.transpose(log_sums, (2, 0, 1)))
    return hand_over(*results)


def solution(mesh):
    finer = Mesh(mesh.devices.reshape(2, 4, 2, 2, 8), AXES)
    rows = P(FSDP, CP, None)
    return jax.shard_map(
        on_device, mesh=finer, in_specs=(rows,) * 7,
        out_specs=(rows, rows, rows, P(FSDP, CP)), check_vma=False,
    )
```

```python
import functools

import jax
import jax.numpy as jnp
from jax import lax
from jax.experimental import pallas as pl
from jax.experimental.pallas import tpu as pltpu
from jax.sharding import Mesh
from jax.sharding import PartitionSpec as P

AXES = ("x_hi", "y", "core", "x_lo", "z")
FSDP = ("x_hi", "y", "core")
CP = ("x_lo", "z")
LOG2E = 1.4426950408889634
HEADS = 10
HALF = HEADS // 2
SPAN = 128
N_CP = 16
N_Z = 8
MESH = pl.DeviceIdType.MESH
F32 = jnp.float32
BF16 = jnp.bfloat16
NT = (((1,), (1,)), ((), ()))
TN = (((0,), (0,)), ((), ()))


def owner_of(head, parity):
    spare = head >= N_Z
    z = jnp.where(spare, 2 * parity + 4 * (head - N_Z), head)
    x = jnp.where(spare, 1 - parity, lax.rem(head + parity, 2))
    return x, z


def head_of(x, z, parity):
    first = x == lax.rem(z + parity, 2)
    spare = jnp.where(z == 2 * parity, N_Z, jnp.where(z == 2 * parity + 4, N_Z + 1, HEADS))
    return jnp.where(first, z, spare)


def step_kernel(
    f_in, q_in, k_in, v_in, o_in, g_in, l_in, dq_out, dk_out, dv_out, dw_out,
    q_buf, k_buf, v_buf, g_buf, s_buf, prob, dq_acc, done, back,
    g_own, o_own, l_own, s_own, f_own, ft_own, ft_out, ft_buf, dv_buf,
    half_send, half_recv, part, x_send, x_recv, z_send, z_recv, total,
    in_sem, send_sem, recv_sem, pair_sem, ret_send, ret_recv, value_sem, out_sem,
    f_ssem, f_rsem, y_ssem, y_rsem, d_ssem, d_rsem, x_ssem, x_rsem, z_ssem, z_rsem,
    *, scale, rows
):
    xh, y, core = lax.axis_index("x_hi"), lax.axis_index("y"), lax.axis_index("core")
    xl, z = lax.axis_index("x_lo"), lax.axis_index("z")
    x = 2 * xh + xl
    me = 2 * z + xl
    mine = head_of(xl, z, core)
    active = mine < HEADS
    feat = f_in.shape[2]
    half_w = q_in.shape[2] // 2
    blk = feat // 16
    piece = blk // 2
    col = half_w // N_Z

    def cp_id(peer):
        return {"x_lo": lax.rem(peer, 2), "z": peer // 2}

    def row_id(p):
        return {"x_hi": p // 2, "x_lo": lax.rem(p, 2)}

    def y_id(p):
        return {"y": p}

    near, near_id = (y, x), (y_id, row_id)
    across, across_id = (x, y), (row_id, y_id)

    loads = [
        pltpu.make_async_copy(g_in.at[0], g_own, in_sem.at[0]),
        pltpu.make_async_copy(o_in.at[0], o_own, in_sem.at[1]),
        pltpu.make_async_copy(l_in, l_own, in_sem.at[2]),
        pltpu.make_async_copy(f_in.at[0], f_own, in_sem.at[3]),
    ]
    for c in loads:
        c.start()

    barrier = pltpu.get_barrier_semaphore()

    def signal(where):
        pl.semaphore_signal(barrier, inc=1, device_id=where, device_id_type=MESH)

    def greet_cp(j, _):
        signal(cp_id(lax.rem(me + j, N_CP)))
        return 0

    def greet_quad(j, _):
        signal({"y": lax.rem(y + j, 4)})
        signal(row_id(lax.rem(x + j, 4)))
        return 0

    lax.fori_loop(1, N_CP, greet_cp, 0)
    lax.fori_loop(1, 4, greet_quad, 0)
    signal({"core": 1 - core})
    pl.semaphore_wait(barrier, N_CP + 6)

    def far_first(i):
        return jnp.where(lax.rem(i, 2) == 0, 4 + i // 2, 3 - i // 2) % N_Z

    def head_at(i):
        return jnp.where(i < 2, N_Z + i, lax.rem(z + far_first(i - 2), N_Z))

    def cols_of(head):
        return pl.ds(pl.multiple_of(head * SPAN, SPAN), SPAN)

    ins = (k_in, q_in, g_in, v_in)
    bufs = (k_buf, q_buf, g_buf, v_buf)

    def source(t, head):
        return ins[t].at[0, :, cols_of(head)] if t < 4 else s_own.at[head]

    def target(t, block):
        return bufs[t].at[block] if t < 4 else s_buf.at[block]

    def landed(t, b):
        return pair_sem.at[0 if t == 0 else 1, b] if t in (0, 3) else recv_sem.at[t]

    def send_all(kinds):
        def send(i, _):
            head = head_at(i)
            ox, oz = owner_of(head, core)

            @pl.when(head != mine)
            def _():
                for t in kinds:
                    pltpu.make_async_remote_copy(
                        src_ref=source(t, head), dst_ref=target(t, me),
                        send_sem=send_sem.at[t], recv_sem=landed(t, z),
                        device_id={"x_lo": ox, "z": oz}, device_id_type=MESH).start()

            @pl.when(head == mine)
            def _():
                for t in kinds:
                    if t < 4:
                        pltpu.make_async_copy(source(t, head), target(t, me), landed(t, z)).start()
                    else:
                        s_buf[me] = s_own[head]

            return 0

        lax.fori_loop(0, HEADS, send, 0)

    send_all((1, 2))

    for c in loads[:3]:
        c.wait()
    lse = l_own[...] * LOG2E
    s_own[...] = jnp.zeros_like(s_own)
    for h in range(HEADS):
        hs = slice(h * SPAN, (h + 1) * SPAN)
        product = g_own[:, hs].astype(F32) * o_own[:, hs].astype(F32)
        s_own[h, 0:1, :] = lse[h]
        s_own[h, 1:2, :] = jnp.sum(product.T, axis=0, keepdims=True)
    send_all((4,))
    send_all((0,))

    loads[3].wait()

    def turn(i, _):
        at = pl.multiple_of(i * SPAN, SPAN)
        ft_own[pl.ds(at, SPAN), :] = f_own[:, pl.ds(at, SPAN)].T
        return 0

    lax.fori_loop(0, feat // SPAN, turn, 0)

    def sort(i, _):
        f, part_s = i // 2, lax.rem(i, 2)
        of_y, of_x, of_core = lax.rem(f // 2, 4), 2 * (f // 8) + part_s, lax.rem(f, 2)
        value = ft_own[pl.ds(pl.multiple_of(i * piece, piece), piece), :]
        ft_out[0, of_y, pl.ds(pl.multiple_of((of_core * 4 + of_x) * piece, piece), piece), :] = value
        ft_out[1, of_x, pl.ds(pl.multiple_of((of_core * 4 + of_y) * piece, piece), piece), :] = value
        return 0

    lax.fori_loop(0, feat // piece, sort, 0)

    def my_span(w):
        return pl.ds(pl.multiple_of(near[w] * SPAN, SPAN), SPAN)

    def feature_copy(w, j):
        to = lax.rem(near[w] + j, 4)
        return pltpu.make_async_remote_copy(
            src_ref=ft_out.at[w, to], dst_ref=ft_buf.at[w, :, my_span(w)],
            send_sem=f_ssem.at[w, j], recv_sem=f_rsem.at[w, j], device_id=near_id[w](to),
            device_id_type=MESH)

    for w in range(2):
        if w == 0:
            for j in range(1, 4):
                feature_copy(w, j).start()
        ft_buf[w, :, my_span(w)] = ft_out[w, near[w]]

    def gone(ref, sem):
        pltpu.make_async_copy(ref, ref, sem).wait()

    def left(kinds):
        def count(n):
            for t in kinds:
                gone(ins[t].at[0, :, : n * SPAN] if t < 4 else s_own.at[:n], send_sem.at[t])

        pl.when(active)(lambda: count(HEADS - 1))
        pl.when(jnp.logical_not(active))(lambda: count(HEADS))

    left((1, 2))
    for j in range(1, 4):
        feature_copy(1, j).start()
    left((0,))

    def value_copy(w, h, o):
        return pltpu.make_async_remote_copy(
            src_ref=back.at[0, :, cols_of(h)],
            dst_ref=dv_buf.at[w, my_span(w), cols_of(h - HALF * w)],
            send_sem=y_ssem.at[0], recv_sem=y_rsem.at[w, near[w]],
            device_id=near_id[w](lax.rem(near[w] + o, 4)), device_id_type=MESH)

    def pass_on(i, _):
        h = jnp.where(i < N_Z, lax.rem(z + far_first(i), N_Z), i)

        @pl.when(h != mine)
        def _():
            gone(back.at[0, :, cols_of(h)], value_sem.at[h])

        for w in range(2):
            @pl.when(h // HALF == w)
            def _():
                for o in range(1, 4):
                    value_copy(w, h, o).start()
        return 0

    UB = 2
    seq = N_CP * rows

    def block_at(i):
        return lax.rem(z + N_Z - far_first(i), N_Z)

    def arrive_pair(t, b):
        gone(bufs[t].at[pl.ds(2 * b, 2)], landed(t, b))

    def give(t, r):
        @pl.when(r != me)
        def _():
            pltpu.make_async_remote_copy(
                src_ref=done.at[t, r], dst_ref=back.at[t, :, cols_of(mine)],
                send_sem=ret_send.at[t], recv_sem=value_sem.at[mine] if t == 0 else ret_recv.at[t],
                device_id=cp_id(r), device_id_type=MESH).start()

        @pl.when(r == me)
        def _():
            back[t, :, cols_of(mine)] = done[t, me]

    @pl.when(active)
    def _():
        gone(q_buf, recv_sem.at[1])
        gone(g_buf, recv_sem.at[2])
        gone(s_buf.at[: N_CP - 1], recv_sem.at[4])
        lse = jnp.concatenate([s_buf[i, 0:1, :] for i in range(N_CP)], axis=1)

        def value_step(i, _):
            b = block_at(i)
            us = pl.ds(b * UB, UB)
            arrive_pair(0, b)
            k = k_buf[us].reshape(UB * rows, SPAN)
            st = lax.dot_general(k, q_buf[...].reshape(seq, SPAN), NT, preferred_element_type=F32)
            p = jnp.exp2(st * (scale * LOG2E) - lse)
            prob[pl.ds(pl.multiple_of(b * UB * rows, UB * rows), UB * rows), :] = p
            dv = jnp.dot(p.astype(BF16), g_buf[...].reshape(seq, SPAN), preferred_element_type=F32)
            done[0, us] = dv.astype(BF16).reshape(UB, rows, SPAN)
            give(0, 2 * b)
            give(0, 2 * b + 1)
            return 0

        lax.fori_loop(0, N_CP // UB, value_step, 0)
        dq_acc[...] = jnp.zeros_like(dq_acc)


    def key_step(i):
        b = block_at(i)
        us = pl.ds(b * UB, UB)
        arrive_pair(3, b)
        k = k_buf[us].reshape(UB * rows, SPAN)
        v = v_buf[us].reshape(UB * rows, SPAN)
        delta = jnp.concatenate([s_buf[i, 1:2, :] for i in range(N_CP)], axis=1)
        p = prob[pl.ds(pl.multiple_of(b * UB * rows, UB * rows), UB * rows), :]
        dp = lax.dot_general(v, g_buf[...].reshape(seq, SPAN), NT, preferred_element_type=F32)
        ds = (p * (dp - delta)).astype(BF16)
        dk = jnp.dot(ds, q_buf[...].reshape(seq, SPAN), preferred_element_type=F32)
        done[1, us] = (dk * scale).astype(BF16).reshape(UB, rows, SPAN)
        dq_acc[...] += lax.dot_general(k, ds, TN, preferred_element_type=F32)
        give(1, 2 * b)
        give(1, 2 * b + 1)

    def key_steps(lo, hi):
        def one(i, _):
            @pl.when(active)
            def _():
                key_step(i)
            return 0

        lax.fori_loop(lo, hi, one, 0)

    def finish_queries():
        def query_give(i, _):
            b = block_at(i)
            cs = pl.ds(pl.multiple_of(b * UB * rows, UB * rows), UB * rows)
            turned = (dq_acc[:, cs].T * scale).astype(BF16)
            done[2, pl.ds(b * UB, UB)] = turned.reshape(UB, rows, SPAN)
            give(2, 2 * b)
            give(2, 2 * b + 1)
            return 0

        lax.fori_loop(0, N_Z, query_give, 0)

    def passes(lo, hi):
        lax.fori_loop(lo, hi, pass_on, 0)

    send_all((3,))
    passes(0, HEADS)
    key_steps(0, N_Z)
    pl.when(active)(finish_queries)

    outs = (dv_out, dk_out, dq_out)

    def collect_all(t):
        pl.when(active)(lambda: gone(back.at[t, :, : (HEADS - 1) * SPAN], ret_recv.at[t]))
        pl.when(jnp.logical_not(active))(lambda: gone(back.at[t], ret_recv.at[t]))
        pltpu.make_async_copy(back.at[t], outs[t].at[0], out_sem.at[t]).start()

    pltpu.make_async_copy(back.at[0], outs[0].at[0], out_sem.at[0]).start()

    for w in range(2):
        dv_buf[w, my_span(w), :] = back[0, :, w * half_w : (w + 1) * half_w]
    for w in range(2):
        for j in range(1, 4):
            feature_copy(w, j).wait()

    def values_from(w):
        for o in range(1, 4):
            peer = lax.rem(near[w] + o, 4)
            gone(dv_buf.at[w, pl.ds(pl.multiple_of(peer * SPAN, SPAN), SPAN), :], y_rsem.at[w, peer])

    def part_of(w, which):
        rs = pl.ds(pl.multiple_of(which * 2 * blk, 2 * blk), 2 * blk)
        return jnp.dot(ft_buf[w, rs, :], dv_buf[w], preferred_element_type=F32)

    def half_copy(w):
        return pltpu.make_async_remote_copy(
            src_ref=half_send.at[w], dst_ref=half_recv.at[w], send_sem=d_ssem.at[w],
            recv_sem=d_rsem.at[w], device_id={"core": 1 - core}, device_id_type=MESH)

    def across_copy(w, j):
        return pltpu.make_async_remote_copy(
            src_ref=x_send.at[w, j], dst_ref=x_recv.at[w, across[w]], send_sem=x_ssem.at[w, j],
            recv_sem=x_rsem.at[w, across[w]], device_id=across_id[w](j), device_id_type=MESH)

    for w in range(2):
        values_from(w)
        half_send[w] = part_of(w, 1 - core).astype(BF16)
        half_copy(w).start()
        part[...] = part_of(w, core)
        half_copy(w).wait_recv()
        both = (part[...] + half_recv[w].astype(F32)).astype(BF16)
        x_send[w] = both.reshape(4, piece, half_w)
        for o in range(1, 4):
            across_copy(w, lax.rem(across[w] + o, 4)).start()
        x_recv[w, across[w]] = x_send[w, across[w]]

    def z_copy(w, zz):
        return pltpu.make_async_remote_copy(
            src_ref=z_send.at[w, zz], dst_ref=z_recv.at[xl, z], send_sem=z_ssem.at[w],
            recv_sem=z_rsem.at[xl], device_id={"x_lo": w, "z": zz}, device_id_type=MESH)

    def is_here(w, zz):
        return jnp.logical_and(xl == w, zz == z)

    gap = jnp.zeros((piece, SPAN - col), BF16)
    for w in range(2):
        for o in range(1, 4):
            s = lax.rem(across[w] + o, 4)
            pltpu.make_async_copy(x_send.at[w, s], x_recv.at[w, s], x_rsem.at[w, s]).wait()
        both = x_recv[w, 0].astype(F32)
        for s in range(1, 4):
            both += x_recv[w, s].astype(F32)
        for zz in range(N_Z):
            block16 = both[:, zz * col : (zz + 1) * col].astype(BF16)
            z_send[w, zz] = jnp.concatenate([block16, gap], axis=1)

        def z_start(i, _):
            zz = lax.rem(z + far_first(i), N_Z)

            @pl.when(jnp.logical_not(is_here(w, zz)))
            def _():
                z_copy(w, zz).start()

            @pl.when(is_here(w, zz))
            def _():
                z_recv[xl, zz] = z_send[w, zz]
            return 0

        lax.fori_loop(0, N_Z, z_start, 0)

    collect_all(1)
    collect_all(2)
    left((4, 3))
    @pl.when(active)
    def _():
        for t in range(3):
            gone(done.at[t, : N_CP - 1], ret_send.at[t])

    gone(dv_buf.at[:, : 3 * SPAN], y_ssem.at[0])
    for w in range(2):
        half_copy(w).wait_send()
        for o in range(1, 4):
            across_copy(w, lax.rem(across[w] + o, 4)).wait_send()

    def all_blocks(buf, side, sem):
        pl.when(xl == side)(lambda: gone(buf.at[side, : N_Z - 1], sem.at[side]))
        pl.when(xl != side)(lambda: gone(buf.at[side], sem.at[side]))

    for xs in range(2):
        all_blocks(z_recv, xs, z_rsem)
        rs = slice(xs * piece, (xs + 1) * piece)
        total[rs] = sum(z_recv[xs, zz][:, :col].astype(F32) for zz in range(N_Z))
    last = pltpu.make_async_copy(total, dw_out, out_sem.at[3])
    last.start()

    for w in range(2):
        all_blocks(z_send, w, z_ssem)
    for t in range(3):
        pltpu.make_async_copy(back.at[t], outs[t].at[0], out_sem.at[t]).wait()
    last.wait()


def hand_over_kernel(*refs):
    ins, outs, bufs, sems = refs[:4], refs[4:8], refs[8:12], refs[12]
    first = [pltpu.make_async_copy(a, b, sems.at[0, i]) for i, (a, b) in enumerate(zip(ins, bufs))]
    then = [pltpu.make_async_copy(b, a, sems.at[1, i]) for i, (a, b) in enumerate(zip(outs, bufs))]
    for c in first:
        c.start()
    for c, d in zip(first, then):
        c.wait()
        d.start()
    for d in then:
        d.wait()


def hand_over(*arrays):
    any_spec = pl.BlockSpec(memory_space=pl.ANY)
    return pl.pallas_call(
        hand_over_kernel,
        out_shape=tuple(jax.ShapeDtypeStruct(a.shape, a.dtype) for a in arrays),
        in_specs=[any_spec] * 4,
        out_specs=(any_spec,) * 4,
        scratch_shapes=[pltpu.VMEM(a.shape, a.dtype) for a in arrays]
        + [pltpu.SemaphoreType.DMA((2, 4))],
        name="hand_over",
    )(*arrays)


def on_device(features, query_rows, key_rows, value_rows, attn_output, grad_output, log_sums):
    _, rows, width = query_rows.shape
    feat = features.shape[2]
    seq = N_CP * rows
    blk, half_w = feat // 16, width // 2
    any_spec = pl.BlockSpec(memory_space=pl.ANY)
    block = pltpu.VMEM((N_CP, rows, SPAN), BF16)
    out = jax.ShapeDtypeStruct(query_rows.shape, BF16)
    dma = pltpu.SemaphoreType.DMA
    results = pl.pallas_call(
        functools.partial(step_kernel, scale=SPAN**-0.5, rows=rows),
        out_shape=(out, out, out, jax.ShapeDtypeStruct((blk, half_w // N_Z), F32)),
        in_specs=[any_spec] * 7,
        out_specs=(any_spec,) * 4,
        scratch_shapes=[
            block, block, block, block,
            pltpu.VMEM((N_CP, 8, rows), F32),
            pltpu.VMEM((seq, seq), F32),
            pltpu.VMEM((SPAN, seq), F32),
            pltpu.VMEM((3, N_CP, rows, SPAN), BF16),
            pltpu.VMEM((3, rows, width), BF16),
            pltpu.VMEM((rows, width), BF16),
            pltpu.VMEM((rows, width), BF16),
            pltpu.VMEM((HEADS, 1, rows), F32),
            pltpu.VMEM((HEADS, 8, rows), F32),
            pltpu.VMEM((rows, feat), BF16),
            pltpu.VMEM((feat, rows), BF16),
            pltpu.VMEM((2, 4, feat // 4, rows), BF16),
            pltpu.VMEM((2, feat // 4, 4 * rows), BF16),
            pltpu.VMEM((2, 4 * rows, half_w), BF16),
            pltpu.VMEM((2, 2 * blk, half_w), BF16),
            pltpu.VMEM((2, 2 * blk, half_w), BF16),
            pltpu.VMEM((2 * blk, half_w), F32),
            pltpu.VMEM((2, 4, blk // 2, half_w), BF16),
            pltpu.VMEM((2, 4, blk // 2, half_w), BF16),
            pltpu.VMEM((2, N_Z, blk // 2, SPAN), BF16),
            pltpu.VMEM((2, N_Z, blk // 2, SPAN), BF16),
            pltpu.VMEM((blk, half_w // N_Z), F32),
            dma((4,)),
            dma((5,)), dma((5,)), dma((2, N_Z)), dma((3,)), dma((3,)), dma((HEADS,)), dma((4,)),
            dma((2, 4)), dma((2, 4)), dma((1,)), dma((2, 4)), dma((2,)), dma((2,)),
            dma((2, 4)), dma((2, 4)), dma((2,)), dma((2,)),
        ],
        compiler_params=pltpu.CompilerParams(
            collective_id=0, has_side_effects=True, vmem_limit_bytes=60 * 2**20),
        name="step",
    )(features, query_rows, key_rows, value_rows, attn_output, grad_output,
      jnp.transpose(log_sums, (2, 0, 1)))
    return hand_over(*results)


def solution(mesh):
    finer = Mesh(mesh.devices.reshape(2, 4, 2, 2, 8), AXES)
    rows = P(FSDP, CP, None)
    return jax.shard_map(
        on_device, mesh=finer, in_specs=(rows,) * 7,
        out_specs=(rows, rows, rows, P(FSDP, CP)), check_vma=False,
    )
```
